32 devices in a mesh: row: 8 (over z, y), ch: 4 (over x, core).
Axes of the slice: x: 2, y: 2, z: 4, core: 2. Of those that a mesh axis runs over, the one named last changes fastest.
Arguments:
- pair_rep: float32 [64, 64, 128], P(('row', 'ch')), may hold values from -6 to 6
- pair_mask: int32 [64, 64], P(('row', 'ch')), may hold values from 0 to 1, as said below
- ln_in_gain: float32 [128], replicated, may hold values from 0.5 to 1.5
- ln_in_bias: float32 [128], replicated, may hold values from -3 to 3
- w_in: float32 [128, 640], replicated, may hold values from -0.5 to 0.5
- b_in: float32 [640], replicated, may hold values from -3 to 3
- ln_out_gain: float32 [128], replicated, may hold values from 0.5 to 1.5
- ln_out_bias: float32 [128], replicated, may hold values from -3 to 3
- w_out: float32 [128, 128], replicated, may hold values from -0.5 to 0.5
- b_out: float32 [128], replicated, may hold values from -3 to 3
- cotangent: float32 [64, 64, 128], P(('row', 'ch')), may hold values from -6 to 6
Outputs:
- update: float32 [64, 64, 128], P(('row', 'ch'))
- grad_pair: float32 [64, 64, 128], P(('row', 'ch'))
- grad_w_in: float32 [128, 640], replicated
- grad_w_out: float32 [128, 128], replicated
The draws below stay inside these ranges and needn't reach their ends.
Inputs may be any that keep to these rules, and one draw needn't show every extreme that they name: pair_mask[i, k] = m_i m_k, where m is 1 for the residues present in the crop and 0 otherwise.
All inputs are finite; a program needn't handle non-finite values.
Results may differ from the reference program's by a relative error of at most 0.00009.
Values sent between devices are 32-bit elements; how exact they have to be, the bound alone decides.
A program may use at most 64 MiB of HBM per device.

```python
import jax
import jax.numpy as jnp
from jax import lax

C = 128
H = 128
N = 64
N_ROW = 8
N_CH = 4


def draw_pair_mask(key, part):
    residue = jax.random.randint(key, (N,), 0, 8)
    present = (residue > 0).astype(jnp.int32)
    return present[:, None] * present[None, :]


def block_scale(rng, extent, cuts, low, top_value):
    def one(axis_at, parts):
        draws = jax.random.uniform(jax.random.fold_in(jax.random.fold_in(rng, 6), axis_at), (parts,), jnp.float32, low / len(cuts), top_value / len(cuts))
        return jnp.repeat(jnp.exp(draws), extent[axis_at] // parts).reshape((-1,) + (1,) * (len(extent) - axis_at - 1))

    gain = one(*cuts[0])
    for cut in cuts[1:]:
        gain = gain * one(*cut)
    return gain


def scatter_about(key, extent, scale, most, split=(), kind=jnp.bfloat16):
    factor_of = block_scale(key, extent, split, -0.22, 0.18) if split else 1.0
    values = jax.random.normal(key, extent, jnp.float32) * scale * factor_of
    return jnp.minimum(jnp.maximum(values, -most), most).astype(kind)


def setup_inputs(seed: int = 0) -> dict:
    arg_keys = jax.random.split(jax.random.key(seed), 12)
    pair_rep = scatter_about(arg_keys[0], (N, N, C), 1.0, 6.0, ((0, 32),), jnp.float32)
    pair_mask = draw_pair_mask(jax.random.fold_in(arg_keys[11], 71), 0)
    ln_in_gain = jnp.clip(jax.random.uniform(arg_keys[2], (C,), jnp.float32, 0.5, 1.5), 0.5, 1.5)
    ln_in_bias = scatter_about(arg_keys[3], (C,), 0.5, 3.0, (), jnp.float32)
    w_in = scatter_about(arg_keys[4], (C, 4 * H + C), C ** -0.5, 0.5, (), jnp.float32)
    b_in = scatter_about(arg_keys[5], (4 * H + C,), 0.5, 3.0, (), jnp.float32)
    ln_out_gain = jnp.clip(jax.random.uniform(arg_keys[6], (H,), jnp.float32, 0.5, 1.5), 0.5, 1.5)
    ln_out_bias = scatter_about(arg_keys[7], (H,), 0.5, 3.0, (), jnp.float32)
    w_out = scatter_about(arg_keys[8], (H, C), H ** -0.5, 0.5, (), jnp.float32)
    b_out = scatter_about(arg_keys[9], (C,), 0.5, 3.0, (), jnp.float32)
    cotangent = scatter_about(arg_keys[10], (N, N, C), 1.0, 6.0, ((0, 32),), jnp.float32)
    return {"pair_rep": pair_rep, "pair_mask": pair_mask, "ln_in_gain": ln_in_gain, "ln_in_bias": ln_in_bias, "w_in": w_in, "b_in": b_in, "ln_out_gain": ln_out_gain, "ln_out_bias": ln_out_bias, "w_out": w_out, "b_out": b_out, "cotangent": cotangent}


epsilon = 1e-05

def prelude(field, keep_mask, norm_gain, norm_bias, weights, offsets):
    channels = field.shape[-1]
    hidden = (weights.shape[1] - channels) // 4
    center = lax.optimization_barrier(jnp.mean(field, -1, keepdims=True))
    spread = lax.optimization_barrier(jnp.mean((field - center) ** 2, -1, keepdims=True))
    normed = (field - center) * lax.rsqrt(spread + epsilon) * norm_gain + norm_bias
    pieces = jnp.einsum('ikc,cf->fik', normed, weights[:, :4 * hidden], precision=lax.Precision.HIGHEST)
    pieces = pieces + offsets[:4 * hidden, None, None]
    gate = jax.nn.sigmoid(jnp.einsum('ikc,cf->ikf', normed, weights[:, 4 * hidden:], precision=lax.Precision.HIGHEST) + offsets[4 * hidden:])
    keep = keep_mask.astype(field.dtype)[None]
    left = keep * jax.nn.sigmoid(pieces[:hidden]) * pieces[hidden:2 * hidden]
    right = keep * jax.nn.sigmoid(pieces[2 * hidden:3 * hidden]) * pieces[3 * hidden:]
    return (left, right, gate)

def epilogue(product, gate, norm_gain, norm_bias, weights, offset):
    center = lax.optimization_barrier(jnp.mean(product, 0, keepdims=True))
    spread = lax.optimization_barrier(jnp.mean((product - center) ** 2, 0, keepdims=True))
    normed = (product - center) * lax.rsqrt(spread + epsilon) * norm_gain[:, None, None] + norm_bias[:, None, None]
    projected = jnp.einsum('hij,hc->ijc', normed, weights, precision=lax.Precision.HIGHEST) + offset
    return gate * projected

def reference(pair_rep, pair_mask, ln_in_gain, ln_in_bias, w_in, b_in, ln_out_gain, ln_out_bias, w_out, b_out, cotangent):
    count = N_ROW * N_CH
    row_count = N // count
    field_blocks = pair_rep.reshape(count, row_count, N, C)
    mask_blocks = pair_mask.reshape(count, row_count, N)

    def forward_block(inputs):
        return prelude(inputs[0], inputs[1], ln_in_gain, ln_in_bias, w_in, b_in)
    left, right, gate = lax.map(forward_block, (field_blocks, mask_blocks))
    left_full = left.transpose(1, 0, 2, 3).reshape(H, N, N)
    right_full = right.transpose(1, 0, 2, 3).reshape(H, N, N)
    product = jnp.einsum('hik,hjk->hij', left_full, right_full, precision=lax.Precision.HIGHEST)
    product_blocks = product.reshape(H, count, row_count, N).transpose(1, 0, 2, 3)
    cot_blocks = cotangent.reshape(count, row_count, N, C)

    def epilogue_block(inputs):

        def local(prod_part, gate_part, weights):
            return epilogue(prod_part, gate_part, ln_out_gain, ln_out_bias, weights, b_out)
        result, backward = jax.vjp(local, inputs[0], inputs[1], w_out)
        d_prod, d_gate, d_weights = backward(inputs[2])
        return (result, d_prod, d_gate, d_weights)
    update, d_product, d_gate, wout_parts = lax.map(epilogue_block, (product_blocks, gate, cot_blocks))
    d_full = d_product.transpose(1, 0, 2, 3).reshape(H, N, N)
    d_left = jnp.einsum('hij,hjk->hik', d_full, right_full, precision=lax.Precision.HIGHEST)
    d_right = jnp.einsum('hij,hik->hjk', d_full, left_full, precision=lax.Precision.HIGHEST)
    d_left = d_left.reshape(H, count, row_count, N).transpose(1, 0, 2, 3)
    d_right = d_right.reshape(H, count, row_count, N).transpose(1, 0, 2, 3)

    def backward_block(inputs):

        def local(field, weights):
            return prelude(field, inputs[1], ln_in_gain, ln_in_bias, weights, b_in)
        _, backward = jax.vjp(local, inputs[0], w_in)
        return backward((inputs[2], inputs[3], inputs[4]))
    grad_blocks, win_parts = lax.map(backward_block, (field_blocks, mask_blocks, d_left, d_right, d_gate))
    grad_pair = grad_blocks.reshape(N, N, C)
    grad_w_in = lax.optimization_barrier(jnp.sum(win_parts, 0)) / N
    grad_w_out = lax.optimization_barrier(jnp.sum(wout_parts, 0)) / N
    return (update.reshape(N, N, C), grad_pair, grad_w_in, grad_w_out)
```

```python
import functools

import jax
import jax.numpy as jnp
from jax import lax
from jax.experimental import pallas as pl
from jax.experimental.pallas import tpu as pltpu
from jax.sharding import PartitionSpec as P

epsilon = 1e-05
MESH = pl.DeviceIdType.MESH


def halves(a):
    high = a.astype(jnp.bfloat16)
    return high, (a - high.astype(jnp.float32)).astype(jnp.bfloat16)


def dot(a, b, contract):
    def one(x, y):
        return lax.dot_general(
            x, y, (contract, ((), ())), preferred_element_type=jnp.float32
        )

    a_high, a_low = halves(a)
    b_high, b_low = halves(b)
    return one(a_high, b_low) + one(a_low, b_high) + one(a_high, b_high)


NN = ((1,), (0,))
NT = ((1,), (1,))
TN = ((0,), (0,))


def normalise(x):
    center = jnp.mean(x, -1, keepdims=True)
    spread = jnp.mean((x - center) ** 2, -1, keepdims=True)
    scale = lax.rsqrt(spread + epsilon)
    return (x - center) * scale, scale


def normalise_back(x_hat, scale, d_hat):
    return scale * (
        d_hat
        - jnp.mean(d_hat, -1, keepdims=True)
        - x_hat * jnp.mean(d_hat * x_hat, -1, keepdims=True)
    )


def farthest_first(n, n_ch):
    assert n & (n - 1) == 0

    def hops(t):
        row, ch = divmod(t, n_ch)
        return (row // 2).bit_length() + row % 2 + ch // 2

    return sorted(range(1, n), key=lambda t: (hops(t), t), reverse=True)


def kernel(
    n_row,
    n_ch,
    *refs,
):
    inputs, rest = refs[:11], refs[11:]
    update_out, gpair_out, recv6, recv8, recv11 = rest[:5]
    held, rest = rest[5:16], rest[16:]
    (
        pair_ref,
        mask_ref,
        gin_ref,
        bin_ref,
        win_ref,
        b_ref,
        gout_ref,
        bout_ref,
        wout_ref,
        bo_ref,
        cot_ref,
    ) = held
    (
        update_ref,
        gpair_ref,
        send1,
        recv1,
        send2,
        recv2,
        send3,
        recv3,
        send4,
        recv4,
        send5,
        recv5,
        send6,
        send7,
        recv7,
        send8,
        send9,
        recv9,
        send10,
        recv10,
        send11,
        send_sems,
        recv_sems,
        load_sems,
        store_sems,
    ) = rest
    n = n_row * n_ch
    rows, length, channels = pair_ref.shape
    hidden = wout_ref.shape[0]
    own = hidden // n
    cells = rows * length
    my_row = lax.axis_index("row")
    my_ch = lax.axis_index("ch")
    me = my_row * n_ch + my_ch

    peers = farthest_first(n, n_ch)

    def place_of(t):
        d = me ^ t
        return d, (d // n_ch, lax.rem(d, n_ch))

    barrier = pltpu.get_barrier_semaphore()
    for t in peers:
        pl.semaphore_signal(barrier, inc=1, device_id=place_of(t)[1], device_id_type=MESH)

    loads = [
        pltpu.make_async_copy(inputs[k], held[k], load_sems.at[k]) for k in range(len(inputs))
    ]
    for k in (0, 2, 3, 4, 5, 1, 10, 6, 7, 8, 9):
        loads[k].start()

    def exchange(phase, src, dst, spread):
        for t in peers:
            d, place = place_of(t)
            pltpu.make_async_remote_copy(
                src_ref=src.at[d] if spread else src,
                dst_ref=dst.at[me],
                send_sem=send_sems.at[phase],
                recv_sem=recv_sems.at[phase],
                device_id=place,
                device_id_type=MESH,
            ).start()
        if spread:
            dst[me] = src[me]

    def arrived(phase, dst):
        part = dst.at[pl.ds(0, n - 1)]
        pltpu.make_async_copy(part, part, recv_sems.at[phase]).wait()

    def sent(phase, dst):
        part = dst.at[pl.ds(0, n - 1)]
        pltpu.make_async_copy(part, part, send_sems.at[phase]).wait()

    def load_cells(ref):
        return jnp.concatenate(
            [ref[i, pl.ds(p, n, stride=rows), :] for i in range(rows) for p in range(rows)], 0
        )

    def store_cells(ref, value):
        for i in range(rows):
            for p in range(rows):
                at = i * length + p * n
                ref[i, pl.ds(p, n, stride=rows), :] = value[at : at + n]

    def split_h(value):
        return value.T.reshape(n, own, cells)

    def merge_h(value):
        return value.reshape(hidden, cells).T

    def stack(value):
        return jnp.concatenate([value[:, i * length : (i + 1) * length] for i in range(rows)], 0)

    def unstack(value):
        return jnp.concatenate([value[i * n : (i + 1) * n] for i in range(rows)], 1)

    def bias(first, last):
        return jnp.concatenate([b_ref[k : k + 1] for k in range(first, last)], 1)

    natural = lax.broadcasted_iota(jnp.int32, (length, length), 0)
    place = lax.broadcasted_iota(jnp.int32, (length, length), 1)
    order = jnp.where(natural == lax.rem(place, n) * rows + place // n, 1.0, 0.0)
    loads[1].wait()
    keep = lax.dot_general(
        mask_ref[...].astype(jnp.bfloat16),
        order.astype(jnp.bfloat16),
        (NN, ((), ())),
        preferred_element_type=jnp.float32,
    )
    keep = jnp.concatenate([keep[i : i + 1] for i in range(rows)], 1)

    loads[0].wait()
    loads[2].wait()
    loads[3].wait()
    pair_hat, pair_scale = normalise(load_cells(pair_ref))
    normed = pair_hat * gin_ref[...] + bin_ref[...]
    width = 4 * hidden
    lanes = b_ref.shape[1]
    loads[4].wait()
    loads[5].wait()
    pieces = dot(normed, win_ref[:, :width], NN) + bias(0, width // lanes)
    p1 = jax.nn.sigmoid(pieces[:, :hidden])
    p2 = pieces[:, hidden : 2 * hidden]
    p3 = jax.nn.sigmoid(pieces[:, 2 * hidden : 3 * hidden])
    p4 = pieces[:, 3 * hidden :]
    keep_tall = jnp.broadcast_to(keep, (hidden, cells)).T
    left = keep_tall * p1 * p2
    right = keep_tall * p3 * p4
    send1[:, :own, :] = split_h(left)
    send1[:, own:, :] = split_h(right)
    pl.semaphore_wait(barrier, n - 1)
    exchange(0, send1, recv1, True)

    gate = jax.nn.sigmoid(dot(normed, win_ref[:, width:], NN) + bias(width // lanes, b_ref.shape[0]))
    for k in range(6, 11):
        loads[k].wait()
    cot = load_cells(cot_ref)

    arrived(0, recv1)
    lefts = [stack(recv1[:, h, :]) for h in range(own)]
    rights = [stack(recv1[:, own + h, :]) for h in range(own)]
    for h in range(own):
        send2[:, h, :] = unstack(dot(lefts[h], rights[h], NT))
    exchange(1, send2, recv2, True)
    arrived(1, recv2)

    prod_hat, prod_scale = normalise(merge_h(recv2[...]))
    normed_product = prod_hat * gout_ref[...] + bout_ref[...]
    projected = dot(normed_product, wout_ref[...], NN) + bo_ref[...]
    d_out = cot * gate
    d_product = normalise_back(
        prod_hat, prod_scale, dot(d_out, wout_ref[...], NT) * gout_ref[...]
    )
    send3[...] = split_h(d_product)
    exchange(2, send3, recv3, True)

    store_cells(update_ref, gate * projected)
    update_copy = pltpu.make_async_copy(update_ref, update_out, store_sems.at[0])
    update_copy.start()
    d_gate = cot * projected * gate * (1.0 - gate)
    d_wout = dot(normed_product, d_out, TN)
    d_wgate = dot(normed, d_gate, TN)
    send4[...] = jnp.concatenate([d_wgate, d_wout], 1).reshape(n, own, channels + channels)
    exchange(3, send4, recv4, True)
    d_normed = dot(d_gate, win_ref[:, width:], NT)

    arrived(2, recv3)
    d_cols = [stack(recv3[:, h, :]) for h in range(own)]
    for h in range(own):
        send5[:, h, :] = unstack(dot(d_cols[h], rights[h], NN))
    exchange(4, send5, recv5, True)
    for h in range(own):
        send9[:, h, :] = unstack(dot(d_cols[h], lefts[h], TN))
    exchange(8, send9, recv9, True)

    arrived(3, recv4)
    send6[...] = jnp.sum(recv4[...], 0) / length
    early_copy = pltpu.make_async_copy(send6, recv6.at[me], store_sems.at[2])
    early_copy.start()
    exchange(5, send6, recv6, False)

    arrived(4, recv5)
    half = 2 * hidden
    d_left = merge_h(recv5[...]) * keep_tall
    d_first = jnp.concatenate([d_left * p2 * p1 * (1.0 - p1), d_left * p1], 1)
    send7[...] = dot(normed, d_first, TN).reshape(n, own, half)
    exchange(6, send7, recv7, True)
    d_normed = d_normed + dot(d_first, win_ref[:, :half], NT)
    arrived(8, recv9)
    d_right = merge_h(recv9[...]) * keep_tall
    d_second = jnp.concatenate([d_right * p4 * p3 * (1.0 - p3), d_right * p3], 1)
    send10[...] = dot(normed, d_second, TN).reshape(n, own, half)
    exchange(9, send10, recv10, True)
    d_normed = d_normed + dot(d_second, win_ref[:, half:width], NT)
    store_cells(gpair_ref, normalise_back(pair_hat, pair_scale, d_normed * gin_ref[...]))
    gpair_copy = pltpu.make_async_copy(gpair_ref, gpair_out, store_sems.at[1])
    gpair_copy.start()
    arrived(6, recv7)
    send8[...] = jnp.sum(recv7[...], 0) / length
    exchange(7, send8, recv8, False)
    late_copy = pltpu.make_async_copy(send8, recv8.at[me], store_sems.at[3])
    late_copy.start()
    arrived(9, recv10)
    send11[...] = jnp.sum(recv10[...], 0) / length
    exchange(10, send11, recv11, False)
    last_copy = pltpu.make_async_copy(send11, recv11.at[me], store_sems.at[4])
    last_copy.start()

    arrived(5, recv6)
    arrived(7, recv8)
    arrived(10, recv11)
    for copy in (update_copy, gpair_copy, early_copy, late_copy, last_copy):
        copy.wait()
    sent(0, recv1)
    sent(1, recv2)
    sent(2, recv3)
    sent(3, recv4)
    sent(4, recv5)
    sent(5, recv6)
    sent(6, recv7)
    sent(7, recv8)
    sent(8, recv9)
    sent(9, recv10)
    sent(10, recv11)


def finish(update, gpair, early, late, last, update_ref, gpair_ref, gwin_ref, gwout_ref):
    channels = gwin_ref.shape[0]
    width = late.shape[2]
    update_ref[...] = update[...]
    gpair_ref[...] = gpair[...]
    early_rows = early[...].reshape(channels, 2 * channels)
    gwin_ref[:, 2 * width :] = early_rows[:, :channels]
    gwout_ref[...] = early_rows[:, channels:]
    gwin_ref[:, :width] = late[...].reshape(channels, width)
    gwin_ref[:, width : 2 * width] = last[...].reshape(channels, width)


def on_device(
    n_row,
    n_ch,
    pair_rep,
    pair_mask,
    ln_in_gain,
    ln_in_bias,
    w_in,
    b_in,
    ln_out_gain,
    ln_out_bias,
    w_out,
    b_out,
    cotangent,
):
    n = n_row * n_ch
    rows, length, channels = pair_rep.shape
    hidden = w_out.shape[0]
    own = hidden // n
    cells = rows * length
    f32 = jnp.float32

    def both(*shape):
        return [pltpu.VMEM((n, *shape), f32), pltpu.VMEM((n, *shape), f32)]

    inputs = (
        pair_rep,
        pair_mask,
        ln_in_gain[None],
        ln_in_bias[None],
        w_in,
        b_in.reshape(-1, min(128, hidden)),
        ln_out_gain[None],
        ln_out_bias[None],
        w_out,
        b_out[None],
        cotangent,
    )
    anywhere = pl.BlockSpec(memory_space=pl.ANY)
    parts = pl.pallas_call(
        functools.partial(kernel, n_row, n_ch),
        out_shape=(
            jax.ShapeDtypeStruct(pair_rep.shape, f32),
            jax.ShapeDtypeStruct(pair_rep.shape, f32),
            jax.ShapeDtypeStruct((n, own, 2 * channels), f32),
            jax.ShapeDtypeStruct((n, own, 2 * hidden), f32),
            jax.ShapeDtypeStruct((n, own, 2 * hidden), f32),
        ),
        in_specs=[anywhere] * 11,
        out_specs=(anywhere,) * 5,
        scratch_shapes=[
            *[pltpu.VMEM(x.shape, x.dtype) for x in inputs],
            pltpu.VMEM(pair_rep.shape, f32),
            pltpu.VMEM(pair_rep.shape, f32),
            *both(2 * own, cells),
            *both(own, cells),
            *both(own, cells),
            *both(own, 2 * channels),
            *both(own, cells),
            pltpu.VMEM((own, 2 * channels), f32),
            *both(own, 2 * hidden),
            pltpu.VMEM((own, 2 * hidden), f32),
            *both(own, cells),
            *both(own, 2 * hidden),
            pltpu.VMEM((own, 2 * hidden), f32),
            pltpu.SemaphoreType.DMA((11,)),
            pltpu.SemaphoreType.DMA((11,)),
            pltpu.SemaphoreType.DMA((11,)),
            pltpu.SemaphoreType.DMA((5,)),
        ],
        compiler_params=pltpu.CompilerParams(collective_id=0, has_side_effects=True),
    )(*inputs)
    vmem = pl.BlockSpec(memory_space=pltpu.VMEM)
    return pl.pallas_call(
        finish,
        out_shape=(
            jax.ShapeDtypeStruct(pair_rep.shape, f32),
            jax.ShapeDtypeStruct(pair_rep.shape, f32),
            jax.ShapeDtypeStruct(w_in.shape, f32),
            jax.ShapeDtypeStruct(w_out.shape, f32),
        ),
        in_specs=[vmem] * 5,
        out_specs=(vmem,) * 4,
    )(*parts)


def solution(mesh):
    rows = P(("row", "ch"), None, None)
    placed = (rows, P(("row", "ch"), None), P(), P(), P(), P(), P(), P(), P(), P(), rows)
    return jax.shard_map(
        functools.partial(on_device, mesh.shape["row"], mesh.shape["ch"]),
        mesh=mesh,
        in_specs=placed,
        out_specs=(rows, rows, P(), P()),
        check_vma=False,
    )
```

```python
import functools

import jax
import jax.numpy as jnp
from jax import lax
from jax.experimental import pallas as pl
from jax.experimental.pallas import tpu as pltpu
from jax.sharding import PartitionSpec as P

epsilon = 1e-05
MESH = pl.DeviceIdType.MESH


def halves(a):
    high = a.astype(jnp.bfloat16)
    return high, (a - high.astype(jnp.float32)).astype(jnp.bfloat16)


def dot(a, b, contract):
    def one(x, y):
        return lax.dot_general(
            x, y, (contract, ((), ())), preferred_element_type=jnp.float32
        )

    a_high, a_low = halves(a)
    b_high, b_low = halves(b)
    return one(a_high, b_low) + one(a_low, b_high) + one(a_high, b_high)


NN = ((1,), (0,))
NT = ((1,), (1,))
TN = ((0,), (0,))


def normalise(x):
    center = jnp.mean(x, -1, keepdims=True)
    spread = jnp.mean((x - center) ** 2, -1, keepdims=True)
    scale = lax.rsqrt(spread + epsilon)
    return (x - center) * scale, scale


def normalise_back(x_hat, scale, d_hat):
    return scale * (
        d_hat
        - jnp.mean(d_hat, -1, keepdims=True)
        - x_hat * jnp.mean(d_hat * x_hat, -1, keepdims=True)
    )


def farthest_first(n, n_ch):
    assert n & (n - 1) == 0

    def hops(t):
        row, ch = divmod(t, n_ch)
        return (row // 2).bit_length() + row % 2 + ch // 2

    return sorted(range(1, n), key=lambda t: (hops(t), t), reverse=True)


def kernel(
    n_row,
    n_ch,
    *refs,
):
    inputs, rest = refs[:11], refs[11:]
    update_ref, gpair_ref, gwin_out, gwout_out = rest[:4]
    held, rest = rest[4:15], rest[15:]
    (
        pair_ref,
        mask_ref,
        gin_ref,
        bin_ref,
        win_ref,
        b_ref,
        gout_ref,
        bout_ref,
        wout_ref,
        bo_ref,
        cot_ref,
    ) = held
    (
        recv6, recv8, recv11,
        send1,
        recv1,
        send2,
        recv2,
        send3,
        recv3,
        send4,
        recv4,
        send5,
        recv5,
        send6,
        send7,
        recv7,
        send8,
        send9,
        recv9,
        send10,
        recv10,
        send11,
        send_sems,
        recv_sems,
        load_sems,
        store_sems,
    ) = rest
    n = n_row * n_ch
    rows, length, channels = pair_ref.shape
    hidden = wout_ref.shape[0]
    own = hidden // n
    cells = rows * length
    my_row = lax.axis_index("row")
    my_ch = lax.axis_index("ch")
    me = my_row * n_ch + my_ch

    peers = farthest_first(n, n_ch)

    def place_of(t):
        d = me ^ t
        return d, (d // n_ch, lax.rem(d, n_ch))

    barrier = pltpu.get_barrier_semaphore()
    for t in peers:
        pl.semaphore_signal(barrier, inc=1, device_id=place_of(t)[1], device_id_type=MESH)

    loads = [
        pltpu.make_async_copy(inputs[k], held[k], load_sems.at[k]) for k in range(len(inputs))
    ]
    for k in (0, 2, 3, 4, 5, 1, 10, 6, 7, 8, 9):
        loads[k].start()

    def exchange(phase, src, dst, spread):
        for t in peers:
            d, place = place_of(t)
            pltpu.make_async_remote_copy(
                src_ref=src.at[d] if spread else src,
                dst_ref=dst.at[me],
                send_sem=send_sems.at[phase],
                recv_sem=recv_sems.at[phase],
                device_id=place,
                device_id_type=MESH,
            ).start()
        if spread:
            dst[me] = src[me]

    def arrived(phase, dst):
        part = dst.at[pl.ds(0, n - 1)]
        pltpu.make_async_copy(part, part, recv_sems.at[phase]).wait()

    def sent(phase, dst):
        part = dst.at[pl.ds(0, n - 1)]
        pltpu.make_async_copy(part, part, send_sems.at[phase]).wait()

    def load_cells(ref):
        return jnp.concatenate(
            [ref[i, pl.ds(p, n, stride=rows), :] for i in range(rows) for p in range(rows)], 0
        )

    def store_cells(ref, value):
        for i in range(rows):
            for p in range(rows):
                at = i * length + p * n
                ref[i, pl.ds(p, n, stride=rows), :] = value[at : at + n]

    def split_h(value):
        return value.T.reshape(n, own, cells)

    def merge_h(value):
        return value.reshape(hidden, cells).T

    def stack(value):
        return jnp.concatenate([value[:, i * length : (i + 1) * length] for i in range(rows)], 0)

    def unstack(value):
        return jnp.concatenate([value[i * n : (i + 1) * n] for i in range(rows)], 1)

    def bias(first, last):
        return jnp.concatenate([b_ref[k : k + 1] for k in range(first, last)], 1)

    natural = lax.broadcasted_iota(jnp.int32, (length, length), 0)
    place = lax.broadcasted_iota(jnp.int32, (length, length), 1)
    order = jnp.where(natural == lax.rem(place, n) * rows + place // n, 1.0, 0.0)
    loads[1].wait()
    keep = lax.dot_general(
        mask_ref[...].astype(jnp.bfloat16),
        order.astype(jnp.bfloat16),
        (NN, ((), ())),
        preferred_element_type=jnp.float32,
    )
    keep = jnp.concatenate([keep[i : i + 1] for i in range(rows)], 1)

    loads[0].wait()
    loads[2].wait()
    loads[3].wait()
    pair_hat, pair_scale = normalise(load_cells(pair_ref))
    normed = pair_hat * gin_ref[...] + bin_ref[...]
    width = 4 * hidden
    lanes = b_ref.shape[1]
    loads[4].wait()
    loads[5].wait()
    pieces = dot(normed, win_ref[:, :width], NN) + bias(0, width // lanes)
    p1 = jax.nn.sigmoid(pieces[:, :hidden])
    p2 = pieces[:, hidden : 2 * hidden]
    p3 = jax.nn.sigmoid(pieces[:, 2 * hidden : 3 * hidden])
    p4 = pieces[:, 3 * hidden :]
    keep_tall = jnp.broadcast_to(keep, (hidden, cells)).T
    left = keep_tall * p1 * p2
    right = keep_tall * p3 * p4
    send1[:, :own, :] = split_h(left)
    send1[:, own:, :] = split_h(right)
    pl.semaphore_wait(barrier, n - 1)
    exchange(0, send1, recv1, True)

    gate = jax.nn.sigmoid(dot(normed, win_ref[:, width:], NN) + bias(width // lanes, b_ref.shape[0]))
    for k in range(6, 11):
        loads[k].wait()
    cot = load_cells(cot_ref)

    arrived(0, recv1)
    lefts = [stack(recv1[:, h, :]) for h in range(own)]
    rights = [stack(recv1[:, own + h, :]) for h in range(own)]
    for h in range(own):
        send2[:, h, :] = unstack(dot(lefts[h], rights[h], NT))
    exchange(1, send2, recv2, True)
    arrived(1, recv2)

    prod_hat, prod_scale = normalise(merge_h(recv2[...]))
    normed_product = prod_hat * gout_ref[...] + bout_ref[...]
    projected = dot(normed_product, wout_ref[...], NN) + bo_ref[...]
    d_out = cot * gate
    d_product = normalise_back(
        prod_hat, prod_scale, dot(d_out, wout_ref[...], NT) * gout_ref[...]
    )
    send3[...] = split_h(d_product)
    exchange(2, send3, recv3, True)

    store_cells(update_ref, gate * projected)
    d_gate = cot * projected * gate * (1.0 - gate)
    d_wout = dot(normed_product, d_out, TN)
    d_wgate = dot(normed, d_gate, TN)
    send4[...] = jnp.concatenate([d_wgate, d_wout], 1).reshape(n, own, channels + channels)
    exchange(3, send4, recv4, True)
    d_normed = dot(d_gate, win_ref[:, width:], NT)

    arrived(2, recv3)
    d_cols = [stack(recv3[:, h, :]) for h in range(own)]
    for h in range(own):
        send5[:, h, :] = unstack(dot(d_cols[h], rights[h], NN))
    exchange(4, send5, recv5, True)
    for h in range(own):
        send9[:, h, :] = unstack(dot(d_cols[h], lefts[h], TN))
    exchange(8, send9, recv9, True)

    arrived(3, recv4)
    send6[...] = jnp.sum(recv4[...], 0) / length
    recv6[me] = send6[...]
    exchange(5, send6, recv6, False)

    arrived(4, recv5)
    half = 2 * hidden
    d_left = merge_h(recv5[...]) * keep_tall
    d_first = jnp.concatenate([d_left * p2 * p1 * (1.0 - p1), d_left * p1], 1)
    send7[...] = dot(normed, d_first, TN).reshape(n, own, half)
    exchange(6, send7, recv7, True)
    d_normed = d_normed + dot(d_first, win_ref[:, :half], NT)
    arrived(8, recv9)
    d_right = merge_h(recv9[...]) * keep_tall
    d_second = jnp.concatenate([d_right * p4 * p3 * (1.0 - p3), d_right * p3], 1)
    send10[...] = dot(normed, d_second, TN).reshape(n, own, half)
    exchange(9, send10, recv10, True)
    d_normed = d_normed + dot(d_second, win_ref[:, half:width], NT)
    store_cells(gpair_ref, normalise_back(pair_hat, pair_scale, d_normed * gin_ref[...]))
    arrived(6, recv7)
    send8[...] = jnp.sum(recv7[...], 0) / length
    exchange(7, send8, recv8, False)
    recv8[me] = send8[...]
    arrived(9, recv10)
    send11[...] = jnp.sum(recv10[...], 0) / length
    exchange(10, send11, recv11, False)
    recv11[me] = send11[...]

    arrived(5, recv6)
    arrived(7, recv8)
    arrived(10, recv11)
    finish(None, None, recv6, recv8, recv11, None, None, gwin_out, gwout_out)
    sent(0, recv1)
    sent(1, recv2)
    sent(2, recv3)
    sent(3, recv4)
    sent(4, recv5)
    sent(5, recv6)
    sent(6, recv7)
    sent(7, recv8)
    sent(8, recv9)
    sent(9, recv10)
    sent(10, recv11)


def write_out(a, b, c, d, ao, bo, co, do, sems):
    cs = [pltpu.make_async_copy(x, y, sems.at[k]) for k, (x, y) in enumerate(((a, ao), (b, bo), (c, co), (d, do)))]
    for x in cs:
        x.start()
    for x in cs:
        x.wait()


def finish(update, gpair, early, late, last, update_ref, gpair_ref, gwin_ref, gwout_ref):
    channels = gwin_ref.shape[0]
    width = late.shape[2]
    early_rows = early[...].reshape(channels, 2 * channels)
    gwin_ref[:, 2 * width :] = early_rows[:, :channels]
    gwout_ref[...] = early_rows[:, channels:]
    gwin_ref[:, :width] = late[...].reshape(channels, width)
    gwin_ref[:, width : 2 * width] = last[...].reshape(channels, width)


def on_device(
    n_row,
    n_ch,
    pair_rep,
    pair_mask,
    ln_in_gain,
    ln_in_bias,
    w_in,
    b_in,
    ln_out_gain,
    ln_out_bias,
    w_out,
    b_out,
    cotangent,
):
    n = n_row * n_ch
    rows, length, channels = pair_rep.shape
    hidden = w_out.shape[0]
    own = hidden // n
    cells = rows * length
    f32 = jnp.float32

    def both(*shape):
        return [pltpu.VMEM((n, *shape), f32), pltpu.VMEM((n, *shape), f32)]

    inputs = (
        pair_rep,
        pair_mask,
        ln_in_gain[None],
        ln_in_bias[None],
        w_in,
        b_in.reshape(-1, min(128, hidden)),
        ln_out_gain[None],
        ln_out_bias[None],
        w_out,
        b_out[None],
        cotangent,
    )
    anywhere = pl.BlockSpec(memory_space=pl.ANY)
    inputs = tuple(pltpu.with_memory_space_constraint(x, pltpu.MemorySpace.HBM) for x in inputs)
    parts = pl.pallas_call(
        functools.partial(kernel, n_row, n_ch),
        out_shape=(
            jax.ShapeDtypeStruct(pair_rep.shape, f32),
            jax.ShapeDtypeStruct(pair_rep.shape, f32),
            jax.ShapeDtypeStruct(w_in.shape, f32),
            jax.ShapeDtypeStruct(w_out.shape, f32),
        ),
        in_specs=[anywhere] * 11,
        out_specs=(pl.BlockSpec(memory_space=pltpu.VMEM),) * 4,
        scratch_shapes=[
            *[pltpu.VMEM(x.shape, x.dtype) for x in inputs],
            pltpu.VMEM((n, own, 2 * channels), f32),
            pltpu.VMEM((n, own, 2 * hidden), f32),
            pltpu.VMEM((n, own, 2 * hidden), f32),
            *both(2 * own, cells),
            *both(own, cells),
            *both(own, cells),
            *both(own, 2 * channels),
            *both(own, cells),
            pltpu.VMEM((own, 2 * channels), f32),
            *both(own, 2 * hidden),
            pltpu.VMEM((own, 2 * hidden), f32),
            *both(own, cells),
            *both(own, 2 * hidden),
            pltpu.VMEM((own, 2 * hidden), f32),
            pltpu.SemaphoreType.DMA((11,)),
            pltpu.SemaphoreType.DMA((11,)),
            pltpu.SemaphoreType.DMA((11,)),
            pltpu.SemaphoreType.DMA((5,)),
        ],
        compiler_params=pltpu.CompilerParams(collective_id=0, has_side_effects=True, vmem_limit_bytes=24 << 20),
    )(*inputs)
    return pl.pallas_call(
        write_out,
        out_shape=tuple(jax.ShapeDtypeStruct(x.shape, f32) for x in (pair_rep, pair_rep, w_in, w_out)),
        in_specs=[pl.BlockSpec(memory_space=pltpu.VMEM)] * 4,
        out_specs=(anywhere,) * 4,
        scratch_shapes=[pltpu.SemaphoreType.DMA((4,))],
        compiler_params=pltpu.CompilerParams(vmem_limit_bytes=8 << 20),
    )(*parts)


def solution(mesh):
    rows = P(("row", "ch"), None, None)
    placed = (rows, P(("row", "ch"), None), P(), P(), P(), P(), P(), P(), P(), P(), rows)
    return jax.shard_map(
        functools.partial(on_device, mesh.shape["row"], mesh.shape["ch"]),
        mesh=mesh,
        in_specs=placed,
        out_specs=(rows, rows, P(), P()),
        check_vma=False,
    )
```

```python
import functools

import jax
import jax.numpy as jnp
from jax import lax
from jax.experimental import pallas as pl
from jax.experimental.pallas import tpu as pltpu
from jax.sharding import PartitionSpec as P

epsilon = 1e-05
MESH = pl.DeviceIdType.MESH


def halves(a):
    high = a.astype(jnp.bfloat16)
    return high, (a - high.astype(jnp.float32)).astype(jnp.bfloat16)


def dot_halves(a, b, contract):
    def one(x, y):
        return lax.dot_general(
            x, y, (contract, ((), ())), preferred_element_type=jnp.float32
        )

    (a_high, a_low), (b_high, b_low) = a, b
    return one(a_high, b_low) + one(a_low, b_high) + one(a_high, b_high)


def dot(a, b, contract):
    return dot_halves(halves(a), halves(b), contract)


NN = ((1,), (0,))
NT = ((1,), (1,))
TN = ((0,), (0,))


def normalise(x):
    center = jnp.mean(x, -1, keepdims=True)
    spread = jnp.mean((x - center) ** 2, -1, keepdims=True)
    scale = lax.rsqrt(spread + epsilon)
    return (x - center) * scale, scale


def normalise_back(x_hat, scale, d_hat):
    return scale * (
        d_hat
        - jnp.mean(d_hat, -1, keepdims=True)
        - x_hat * jnp.mean(d_hat * x_hat, -1, keepdims=True)
    )


def farthest_first(n, n_ch):
    assert n & (n - 1) == 0

    def hops(t):
        row, ch = divmod(t, n_ch)
        return (row // 2).bit_length() + row % 2 + ch // 2

    return sorted(range(1, n), key=lambda t: (hops(t), t), reverse=True)


def gather_plan(n, n_ch, rows):
    core, side, up = 1, n_ch // 2, n_ch
    middle = rows // 16 * 8
    plan = []
    for z in range(0, n, 2 * n_ch):
        low = z & -z
        stage = 0 if z == 0 else 1 if z == low else 2
        if stage == 1:
            plan.append((0, 0, z, 0, rows))
        if stage == 2:
            near = z ^ low
            forwards = near & (near - 1) == 0
            plan.append((1, near, low, 0, rows) if forwards else (1, 0, z, 0, rows))
        plan.append((stage, z, side, 0, rows))
        plan.append((stage, z, up, 0, rows))
        if stage < 2:
            plan.append((stage + 1, z ^ side, up, 0, middle))
            plan.append((stage + 1, z ^ up, side, middle, rows))
        else:
            plan.append((stage, z, side ^ up, 0, rows))
        plan.append((stage, z, core, 0, rows))
        plan.append((stage + 1, z ^ side, core, 0, rows))
        plan.append((stage + 1, z ^ up, core, 0, rows))
        plan.append((min(stage + 2, 3), z ^ side ^ up, core, 0, rows))
    return sorted(plan, key=lambda e: (e[0], e[2] == core))


def kernel(
    n_row,
    n_ch,
    plan,
    *refs,
):
    inputs, rest = refs[:11], refs[11:]
    update_ref, gpair_ref, gwin_ref, gwout_ref = rest[:4]
    held, rest = rest[4:15], rest[15:]
    (
        pair_ref,
        mask_ref,
        gin_ref,
        bin_ref,
        win_ref,
        b_ref,
        gout_ref,
        bout_ref,
        wout_ref,
        bo_ref,
        cot_ref,
    ) = held
    (
        send1,
        recv1,
        send2,
        recv2,
        send3,
        recv3,
        send4,
        recv4,
        send5,
        recv5,
        early,
        late,
        blocks,
        weights_t,
        bias_t,
        send_sems,
        recv_sems,
        plan_send,
        plan_recv,
        load_sems,
    ) = rest
    n = n_row * n_ch
    rows, length, channels = pair_ref.shape
    hidden = wout_ref.shape[0]
    own = hidden // n
    cells = rows * length
    my_row = lax.axis_index("row")
    my_ch = lax.axis_index("ch")
    me = my_row * n_ch + my_ch
    peers = farthest_first(n, n_ch)

    def place_of(t):
        d = me ^ t
        return d, (d // n_ch, lax.rem(d, n_ch))

    barrier = pltpu.get_barrier_semaphore()
    for t in peers:
        pl.semaphore_signal(barrier, inc=1, device_id=place_of(t)[1], device_id_type=MESH)

    loads = [
        pltpu.make_async_copy(inputs[k], held[k], load_sems.at[k]) for k in range(len(inputs))
    ]
    for k in (0, 2, 3, 4, 5, 1, 10, 6, 7, 8, 9):
        loads[k].start()

    def exchange(phase, src, dst):
        for t in peers:
            d, place = place_of(t)
            pltpu.make_async_remote_copy(
                src_ref=src.at[d],
                dst_ref=dst.at[me],
                send_sem=send_sems.at[phase],
                recv_sem=recv_sems.at[phase],
                device_id=place,
                device_id_type=MESH,
            ).start()
        dst[me] = src[me]

    def wait_for(sems, phase, ref):
        pltpu.make_async_copy(ref, ref, sems.at[phase]).wait()

    def arrived(phase, dst):
        wait_for(recv_sems, phase, dst.at[pl.ds(0, n - 1)])

    def sent(phase, dst):
        wait_for(send_sems, phase, dst.at[pl.ds(0, n - 1)])

    my_chip = me // 2
    my_core = lax.rem(me, 2)

    def spread(phase, ref):
        for t in peers:
            if t % 2 == 0:
                mine = ref.at[my_chip, my_core]
                pltpu.make_async_remote_copy(
                    src_ref=mine,
                    dst_ref=mine,
                    send_sem=send_sems.at[phase],
                    recv_sem=recv_sems.at[phase],
                    device_id=place_of(t)[1],
                    device_id_type=MESH,
                ).start()

    def same_core(ref):
        return ref.at[pl.ds(0, n // 2 - 1), 0]

    def hand_over(phase, ref):
        mine = ref.at[:, my_core]
        pltpu.make_async_remote_copy(
            src_ref=mine,
            dst_ref=mine,
            send_sem=send_sems.at[phase],
            recv_sem=recv_sems.at[phase],
            device_id=place_of(1)[1],
            device_id_type=MESH,
        ).start()

    def part_of(held_by, first, last):
        return blocks.at[me ^ held_by, pl.ds(first, last - first)]

    here = {0}

    def ensure(block):
        if block in here:
            return
        here.add(block)
        for slot, (_, source, to, first, last) in enumerate(plan):
            if source ^ to == block:
                wait_for(plan_recv, slot, part_of(block, first, last))

    def gather(stage):
        for slot, (when, source, to, first, last) in enumerate(plan):
            if when == stage:
                ensure(source)
                part = part_of(source, first, last)
                pltpu.make_async_remote_copy(
                    src_ref=part,
                    dst_ref=part,
                    send_sem=plan_send.at[slot],
                    recv_sem=plan_recv.at[slot],
                    device_id=place_of(to)[1],
                    device_id_type=MESH,
                ).start()

    def load_cells(ref):
        return jnp.concatenate(
            [ref[i, pl.ds(p, n, stride=rows), :] for i in range(rows) for p in range(rows)], 0
        )

    def store_cells(ref, value):
        for i in range(rows):
            for p in range(rows):
                at = i * length + p * n
                ref[i, pl.ds(p, n, stride=rows), :] = value[at : at + n]

    def split_h(value):
        return value.T.reshape(n, own, cells)

    def merge_h(value):
        return value.reshape(hidden, cells).T

    def stack(value):
        return jnp.concatenate([value[:, i * length : (i + 1) * length] for i in range(rows)], 0)

    def unstack(value):
        return jnp.concatenate([value[i * n : (i + 1) * n] for i in range(rows)], 1)

    def bias(first, last):
        return jnp.concatenate([b_ref[k : k + 1] for k in range(first, last)], 1)

    natural = lax.broadcasted_iota(jnp.int32, (length, length), 0)
    place = lax.broadcasted_iota(jnp.int32, (length, length), 1)
    order = jnp.where(natural == lax.rem(place, n) * rows + place // n, 1.0, 0.0)
    loads[1].wait()
    keep = lax.dot_general(
        mask_ref[...].astype(jnp.bfloat16),
        order.astype(jnp.bfloat16),
        (NN, ((), ())),
        preferred_element_type=jnp.float32,
    )
    keep = jnp.concatenate([keep[i : i + 1] for i in range(rows)], 1)

    loads[0].wait()
    loads[2].wait()
    loads[3].wait()
    pair_hat, pair_scale = normalise(load_cells(pair_ref))
    normed = pair_hat * gin_ref[...] + bin_ref[...]
    width = 4 * hidden
    lanes = b_ref.shape[1]
    loads[4].wait()
    loads[5].wait()
    pieces = dot(normed, win_ref[:, :width], NN) + bias(0, width // lanes)
    p1 = jax.nn.sigmoid(pieces[:, :hidden])
    p2 = pieces[:, hidden : 2 * hidden]
    p3 = jax.nn.sigmoid(pieces[:, 2 * hidden : 3 * hidden])
    p4 = pieces[:, 3 * hidden :]
    keep_tall = jnp.broadcast_to(keep, (hidden, cells)).T
    left = keep_tall * p1 * p2
    right = keep_tall * p3 * p4
    send1[:, :own, :] = split_h(left)
    send1[:, own:, :] = split_h(right)
    blocks[me, :cells, :] = normed
    for q in range(8):
        at = min(q, cells // channels - 1) * channels
        blocks[me, cells + q : cells + q + 1, :] = keep[:, at : at + channels]
    pl.semaphore_wait(barrier, n - 1)
    exchange(0, send1, recv1)
    gather(0)

    for q, k in enumerate((0, 2)):
        at = k * hidden
        weights_t[q] = win_ref[:, at : at + hidden].T.reshape(n, own, channels)
        column = b_ref[at // lanes : at // lanes + 1]
        bias_t[q] = jnp.broadcast_to(column, (lanes, hidden)).T.reshape(n, own, lanes)

    gate = jax.nn.sigmoid(dot(normed, win_ref[:, width:], NN) + bias(width // lanes, b_ref.shape[0]))
    for k in range(6, 11):
        loads[k].wait()
    cot = load_cells(cot_ref)

    arrived(0, recv1)
    lefts = [stack(recv1[:, h, :]) for h in range(own)]
    rights = [stack(recv1[:, own + h, :]) for h in range(own)]
    for h in range(own):
        send2[:, h, :] = unstack(dot(lefts[h], rights[h], NT))
    exchange(1, send2, recv2)
    gather(1)
    arrived(1, recv2)

    prod_hat, prod_scale = normalise(merge_h(recv2[...]))
    normed_product = prod_hat * gout_ref[...] + bout_ref[...]
    projected = dot(normed_product, wout_ref[...], NN) + bo_ref[...]
    d_out = cot * gate
    d_product = normalise_back(
        prod_hat, prod_scale, dot(d_out, wout_ref[...], NT) * gout_ref[...]
    )
    send3[...] = split_h(d_product)
    exchange(2, send3, recv3)

    store_cells(update_ref, gate * projected)
    d_gate = cot * projected * gate * (1.0 - gate)
    d_wout = dot(normed_product, d_out, TN)
    d_wgate = dot(normed, d_gate, TN)
    send4[:, :own, :] = d_wgate.reshape(n, own, channels)
    send4[:, own:, :] = d_wout.reshape(n, own, channels)
    exchange(3, send4, recv4)
    gather(2)
    d_normed = dot(d_gate, win_ref[:, width:], NT)

    arrived(2, recv3)
    d_cols = [stack(recv3[:, h, :]) for h in range(own)]
    for h in range(own):
        send5[:, h, :] = unstack(dot(d_cols[h], rights[h], NN))
    for h in range(own):
        send5[:, own + h, :] = unstack(dot(d_cols[h], lefts[h], TN))
    exchange(4, send5, recv5)
    gather(3)

    arrived(3, recv4)
    early[my_chip, my_core] = jnp.sum(recv4[...], 0) / length
    spread(5, early)
    for block in range(1, n):
        ensure(block)

    group = 8
    gate_weights = halves(jnp.concatenate([weights_t[0, me], weights_t[1, me]], 0))
    gate_bias = jnp.concatenate([bias_t[0, me], bias_t[1, me]], 0)[:, :1]

    def side_by_side(take, first):
        return jnp.concatenate([take(first + i) for i in range(group)], 1)

    def keep_of(d):
        return jnp.concatenate(
            [blocks[d, cells + q : cells + q + 1, :] for q in range(cells // channels)], 1
        )

    def grads_of(g, total):
        first = g * group
        x = jnp.concatenate([blocks[first + i, :cells, :] for i in range(group)], 0)
        x = halves(x)
        gates = jax.nn.sigmoid(dot_halves(gate_weights, x, NT) + gate_bias)
        values = side_by_side(lambda d: recv1[d], first)
        grads = side_by_side(lambda d: send5[d], first)
        present = side_by_side(keep_of, first)
        both = jnp.concatenate([grads * values * (1.0 - gates), grads * present * gates], 0)
        return total + dot_halves(halves(both), x, NN)

    total = lax.fori_loop(
        0, n // group, grads_of, jnp.zeros((4 * own, channels), jnp.float32)
    )
    late[my_chip, my_core] = total / length
    spread(6, late)

    arrived(4, recv5)
    half = 2 * hidden
    d_left = merge_h(recv5[:, :own, :]) * keep_tall
    d_first = jnp.concatenate([d_left * p2 * p1 * (1.0 - p1), d_left * p1], 1)
    d_normed = d_normed + dot(d_first, win_ref[:, :half], NT)
    d_right = merge_h(recv5[:, own:, :]) * keep_tall
    d_second = jnp.concatenate([d_right * p4 * p3 * (1.0 - p3), d_right * p3], 1)
    d_normed = d_normed + dot(d_second, win_ref[:, half:width], NT)
    store_cells(gpair_ref, normalise_back(pair_hat, pair_scale, d_normed * gin_ref[...]))

    wait_for(recv_sems, 5, same_core(early))
    hand_over(7, early)
    wait_for(recv_sems, 6, same_core(late))
    hand_over(8, late)
    wait_for(recv_sems, 7, early.at[:, 0])
    gwin_ref[:, width:] = early[:, :, :own, :].reshape(channels, channels)
    gwout_ref[...] = early[:, :, own:, :].reshape(hidden, channels)
    wait_for(recv_sems, 8, late.at[:, 0])
    for q, k in enumerate((0, 2, 1, 3)):
        piece = late[:, :, q * own : (q + 1) * own, :].reshape(hidden, channels)
        gwin_ref[:, k * hidden : (k + 1) * hidden] = piece.T

    for phase, ref in enumerate((recv1, recv2, recv3, recv4, recv5)):
        sent(phase, ref)
    for phase, ref in ((5, early), (6, late)):
        wait_for(send_sems, phase, same_core(ref))
    for phase, ref in ((7, early), (8, late)):
        wait_for(send_sems, phase, ref.at[:, 0])
    for slot, (_, source, _, first, last) in enumerate(plan):
        wait_for(plan_send, slot, part_of(source, first, last))


def write_out(a, b, c, d, a_out, b_out, c_out, d_out, sems):
    pairs = ((a, a_out), (b, b_out), (c, c_out), (d, d_out))
    copies = [pltpu.make_async_copy(x, y, sems.at[k]) for k, (x, y) in enumerate(pairs)]
    for copy in copies:
        copy.start()
    for copy in copies:
        copy.wait()


def on_device(
    n_row,
    n_ch,
    pair_rep,
    pair_mask,
    ln_in_gain,
    ln_in_bias,
    w_in,
    b_in,
    ln_out_gain,
    ln_out_bias,
    w_out,
    b_out,
    cotangent,
):
    n = n_row * n_ch
    rows, length, channels = pair_rep.shape
    hidden = w_out.shape[0]
    own = hidden // n
    cells = rows * length
    f32 = jnp.float32

    def both(*shape):
        return [pltpu.VMEM((n, *shape), f32), pltpu.VMEM((n, *shape), f32)]

    inputs = (
        pair_rep,
        pair_mask,
        ln_in_gain[None],
        ln_in_bias[None],
        w_in,
        b_in.reshape(-1, min(128, hidden)),
        ln_out_gain[None],
        ln_out_bias[None],
        w_out,
        b_out[None],
        cotangent,
    )
    lanes = min(128, hidden)
    plan = gather_plan(n, n_ch, cells + 8)
    anywhere = pl.BlockSpec(memory_space=pl.ANY)
    vmem = pl.BlockSpec(memory_space=pltpu.VMEM)
    inputs = tuple(pltpu.with_memory_space_constraint(x, pltpu.MemorySpace.HBM) for x in inputs)
    out_shape = tuple(
        jax.ShapeDtypeStruct(x.shape, f32) for x in (pair_rep, pair_rep, w_in, w_out)
    )
    parts = pl.pallas_call(
        functools.partial(kernel, n_row, n_ch, plan),
        out_shape=out_shape,
        in_specs=[anywhere] * 11,
        out_specs=(vmem,) * 4,
        scratch_shapes=[
            *[pltpu.VMEM(x.shape, x.dtype) for x in inputs],
            *both(2 * own, cells),
            *both(own, cells),
            *both(own, cells),
            *both(2 * own, channels),
            *both(2 * own, cells),
            pltpu.VMEM((n // 2, 2, 2 * own, channels), f32),
            pltpu.VMEM((n // 2, 2, 4 * own, channels), f32),
            pltpu.VMEM((n, cells + 8, channels), f32),
            pltpu.VMEM((2, n, own, channels), f32),
            pltpu.VMEM((2, n, own, lanes), f32),
            pltpu.SemaphoreType.DMA((9,)),
            pltpu.SemaphoreType.DMA((9,)),
            pltpu.SemaphoreType.DMA((len(plan),)),
            pltpu.SemaphoreType.DMA((len(plan),)),
            pltpu.SemaphoreType.DMA((11,)),
        ],
        compiler_params=pltpu.CompilerParams(
            collective_id=0, has_side_effects=True, vmem_limit_bytes=56 << 20
        ),
    )(*inputs)
    return pl.pallas_call(
        write_out,
        out_shape=out_shape,
        in_specs=[vmem] * 4,
        out_specs=(anywhere,) * 4,
        scratch_shapes=[pltpu.SemaphoreType.DMA((4,))],
        compiler_params=pltpu.CompilerParams(vmem_limit_bytes=8 << 20),
    )(*parts)


def solution(mesh):
    rows = P(("row", "ch"), None, None)
    placed = (rows, P(("row", "ch"), None), P(), P(), P(), P(), P(), P(), P(), P(), rows)
    return jax.shard_map(
        functools.partial(on_device, mesh.shape["row"], mesh.shape["ch"]),
        mesh=mesh,
        in_specs=placed,
        out_specs=(rows, rows, P(), P()),
        check_vma=False,
    )
```

```python
import functools

import jax
import jax.numpy as jnp
from jax import lax
from jax.experimental import pallas as pl
from jax.experimental.pallas import tpu as pltpu
from jax.sharding import PartitionSpec as P

epsilon = 1e-05
MESH = pl.DeviceIdType.MESH


def halves(a):
    high = a.astype(jnp.bfloat16)
    return high, (a - high.astype(jnp.float32)).astype(jnp.bfloat16)


def dot_halves(a, b, contract):
    def one(x, y):
        return lax.dot_general(
            x, y, (contract, ((), ())), preferred_element_type=jnp.float32
        )

    (a_high, a_low), (b_high, b_low) = a, b
    return one(a_high, b_low) + one(a_low, b_high) + one(a_high, b_high)


def dot(a, b, contract):
    return dot_halves(halves(a), halves(b), contract)


NN = ((1,), (0,))
NT = ((1,), (1,))
TN = ((0,), (0,))


def normalise(x):
    center = jnp.mean(x, -1, keepdims=True)
    spread = jnp.mean((x - center) ** 2, -1, keepdims=True)
    scale = lax.rsqrt(spread + epsilon)
    return (x - center) * scale, scale


def normalise_back(x_hat, scale, d_hat):
    return scale * (
        d_hat
        - jnp.mean(d_hat, -1, keepdims=True)
        - x_hat * jnp.mean(d_hat * x_hat, -1, keepdims=True)
    )


def farthest_first(n, n_ch):
    assert n & (n - 1) == 0

    def hops(t):
        row, ch = divmod(t, n_ch)
        return (row // 2).bit_length() + row % 2 + ch // 2

    return sorted(range(1, n), key=lambda t: (hops(t), t), reverse=True)


def gather_plan(n, n_ch, rows):
    core, side, up = 1, n_ch // 2, n_ch
    middle = rows // 16 * 8
    plan = []
    for z in range(0, n, 2 * n_ch):
        low = z & -z
        stage = 0 if z == 0 else 1 if z == low else 2
        if stage == 1:
            plan.append((0, 0, z, 0, rows))
        if stage == 2:
            near = z ^ low
            forwards = near & (near - 1) == 0
            plan.append((1, near, low, 0, rows) if forwards else (1, 0, z, 0, rows))
        plan.append((stage, z, side, 0, rows))
        plan.append((stage, z, up, 0, rows))
        if stage == 0:
            plan.append((0, 0, side ^ up, 0, rows))
        elif stage < 2:
            plan.append((stage + 1, z ^ side, up, 0, middle))
            plan.append((stage + 1, z ^ up, side, middle, rows))
        else:
            plan.append((1, 0, z ^ side ^ up, 0, rows))
        plan.append((stage, z, core, 0, rows))
        plan.append((stage + 1, z ^ side, core, 0, rows))
        plan.append((stage + 1, z ^ up, core, 0, rows))
        plan.append((1 if z == 0 else min(stage + 2, 3), z ^ side ^ up, core, 0, rows))
    return sorted(plan, key=lambda e: (e[0], e[2] == core))


def kernel(
    n_row,
    n_ch,
    plan,
    *refs,
):
    inputs, rest = refs[:11], refs[11:]
    update_ref, gpair_ref, gwin_ref, gwout_ref = rest[:4]
    held, rest = rest[4:15], rest[15:]
    (
        pair_ref,
        mask_ref,
        gin_ref,
        bin_ref,
        win_ref,
        b_ref,
        gout_ref,
        bout_ref,
        wout_ref,
        bo_ref,
        cot_ref,
    ) = held
    (
        send1,
        recv1,
        send2,
        recv2,
        send3,
        recv3,
        send4,
        pair4,
        sum4,
        recv4,
        send5,
        recv5,
        early,
        late,
        blocks,
        weights_t,
        bias_t,
        send_sems,
        recv_sems,
        plan_send,
        plan_recv,
        load_sems,
    ) = rest
    n = n_row * n_ch
    rows, length, channels = pair_ref.shape
    hidden = wout_ref.shape[0]
    own = hidden // n
    cells = rows * length
    my_row = lax.axis_index("row")
    my_ch = lax.axis_index("ch")
    me = my_row * n_ch + my_ch
    peers = farthest_first(n, n_ch)

    def place_of(t):
        d = me ^ t
        return d, (d // n_ch, lax.rem(d, n_ch))

    barrier = pltpu.get_barrier_semaphore()
    for t in peers:
        pl.semaphore_signal(barrier, inc=1, device_id=place_of(t)[1], device_id_type=MESH)

    loads = [
        pltpu.make_async_copy(inputs[k], held[k], load_sems.at[k]) for k in range(len(inputs))
    ]
    for k in (0, 2, 3, 4, 5, 1, 10, 6, 7, 8, 9):
        loads[k].start()

    def remote(phase, src, dst, to):
        pltpu.make_async_remote_copy(
            src_ref=src,
            dst_ref=dst,
            send_sem=send_sems.at[phase],
            recv_sem=recv_sems.at[phase],
            device_id=place_of(to)[1],
            device_id_type=MESH,
        ).start()

    def exchange(phase, src, dst):
        for t in peers:
            remote(phase, src.at[place_of(t)[0]], dst.at[me], t)
        dst[me] = src[me]

    def wait_for(sems, phase, ref):
        pltpu.make_async_copy(ref, ref, sems.at[phase]).wait()

    def arrived(phase, dst):
        wait_for(recv_sems, phase, dst.at[pl.ds(0, n - 1)])

    def sent(phase, dst):
        wait_for(send_sems, phase, dst.at[pl.ds(0, n - 1)])

    my_chip = me // 2
    my_core = lax.rem(me, 2)

    def spread(phase, ref):
        for t in peers:
            if t % 2 == 0:
                mine = ref.at[my_chip, my_core]
                remote(phase, mine, mine, t)

    def same_core(ref):
        return ref.at[pl.ds(0, n // 2 - 1), 0]

    def hand_over(phase, ref):
        mine = ref.at[:, my_core]
        remote(phase, mine, mine, 1)

    def part_of(held_by, first, last):
        return blocks.at[me ^ held_by, pl.ds(first, last - first)]

    here = {0}

    def ensure(block):
        if block in here:
            return
        here.add(block)
        for slot, (_, source, to, first, last) in enumerate(plan):
            if source ^ to == block:
                wait_for(plan_recv, slot, part_of(block, first, last))

    def gather(stage):
        for slot, (when, source, to, first, last) in enumerate(plan):
            if when == stage:
                ensure(source)
                part = part_of(source, first, last)
                pltpu.make_async_remote_copy(
                    src_ref=part,
                    dst_ref=part,
                    send_sem=plan_send.at[slot],
                    recv_sem=plan_recv.at[slot],
                    device_id=place_of(to)[1],
                    device_id_type=MESH,
                ).start()

    def load_cells(ref):
        return jnp.concatenate(
            [ref[i, pl.ds(p, n, stride=rows), :] for i in range(rows) for p in range(rows)], 0
        )

    def store_cells(ref, value):
        for i in range(rows):
            for p in range(rows):
                at = i * length + p * n
                ref[i, pl.ds(p, n, stride=rows), :] = value[at : at + n]

    def split_h(value):
        return value.T.reshape(n, own, cells)

    def merge_h(value):
        return value.reshape(hidden, cells).T

    def stack(value):
        return jnp.concatenate([value[:, i * length : (i + 1) * length] for i in range(rows)], 0)

    def unstack(value):
        return jnp.concatenate([value[i * n : (i + 1) * n] for i in range(rows)], 1)

    def bias(first, last):
        return jnp.concatenate([b_ref[k : k + 1] for k in range(first, last)], 1)

    natural = lax.broadcasted_iota(jnp.int32, (length, length), 0)
    place = lax.broadcasted_iota(jnp.int32, (length, length), 1)
    order = jnp.where(natural == lax.rem(place, n) * rows + place // n, 1.0, 0.0)
    loads[1].wait()
    keep = lax.dot_general(
        mask_ref[...].astype(jnp.bfloat16),
        order.astype(jnp.bfloat16),
        (NN, ((), ())),
        preferred_element_type=jnp.float32,
    )
    keep = jnp.concatenate([keep[i : i + 1] for i in range(rows)], 1)

    loads[0].wait()
    loads[2].wait()
    loads[3].wait()
    pair_hat, pair_scale = normalise(load_cells(pair_ref))
    normed = pair_hat * gin_ref[...] + bin_ref[...]
    width = 4 * hidden
    lanes = b_ref.shape[1]
    loads[4].wait()
    loads[5].wait()
    pieces = dot(normed, win_ref[:, :width], NN) + bias(0, width // lanes)
    p1 = jax.nn.sigmoid(pieces[:, :hidden])
    p2 = pieces[:, hidden : 2 * hidden]
    p3 = jax.nn.sigmoid(pieces[:, 2 * hidden : 3 * hidden])
    p4 = pieces[:, 3 * hidden :]
    keep_tall = jnp.broadcast_to(keep, (hidden, cells)).T
    left = keep_tall * p1 * p2
    right = keep_tall * p3 * p4
    send1[:, :own, :] = split_h(left)
    send1[:, own:, :] = split_h(right)
    blocks[me, :cells, :] = normed
    for q in range(8):
        at = min(q, cells // channels - 1) * channels
        blocks[me, cells + q : cells + q + 1, :] = keep[:, at : at + channels]
    pl.semaphore_wait(barrier, n - 1)
    exchange(0, send1, recv1)
    gather(0)

    for q, k in enumerate((0, 2)):
        at = k * hidden
        weights_t[q] = win_ref[:, at : at + hidden].T.reshape(n, own, channels)
        column = b_ref[at // lanes : at // lanes + 1]
        bias_t[q] = jnp.broadcast_to(column, (lanes, hidden)).T.reshape(n, own, lanes)

    gate = jax.nn.sigmoid(dot(normed, win_ref[:, width:], NN) + bias(width // lanes, b_ref.shape[0]))
    for k in range(6, 11):
        loads[k].wait()
    cot = load_cells(cot_ref)

    arrived(0, recv1)
    lefts = [stack(recv1[:, h, :]) for h in range(own)]
    rights = [stack(recv1[:, own + h, :]) for h in range(own)]
    for h in range(own):
        send2[:, h, :] = unstack(dot(lefts[h], rights[h], NT))
    exchange(1, send2, recv2)
    gather(1)
    arrived(1, recv2)

    prod_hat, prod_scale = normalise(merge_h(recv2[...]))
    normed_product = prod_hat * gout_ref[...] + bout_ref[...]
    projected = dot(normed_product, wout_ref[...], NN) + bo_ref[...]
    d_out = cot * gate
    d_product = normalise_back(
        prod_hat, prod_scale, dot(d_out, wout_ref[...], NT) * gout_ref[...]
    )
    send3[...] = split_h(d_product)
    exchange(2, send3, recv3)

    store_cells(update_ref, gate * projected)
    d_gate = cot * projected * gate * (1.0 - gate)
    d_wout = dot(normed_product, d_out, TN)
    d_wgate = dot(normed, d_gate, TN)
    send4[:, :, :own, :] = d_wgate.reshape(n // 2, 2, own, channels)
    send4[:, :, own:, :] = d_wout.reshape(n // 2, 2, own, channels)
    remote(9, send4.at[:, 1 - my_core], pair4, 1)
    gather(2)
    d_normed = dot(d_gate, win_ref[:, width:], NT)
    wait_for(recv_sems, 9, pair4)
    sum4[...] = send4[:, my_core] + pair4[...]
    for t in peers:
        if t % 2 == 0:
            remote(3, sum4.at[place_of(t)[0] // 2], recv4.at[my_chip], t)
    recv4[my_chip] = sum4[my_chip]

    arrived(2, recv3)
    d_cols = [stack(recv3[:, h, :]) for h in range(own)]
    for h in range(own):
        send5[:, h, :] = unstack(dot(d_cols[h], rights[h], NN))
    for h in range(own):
        send5[:, own + h, :] = unstack(dot(d_cols[h], lefts[h], TN))
    exchange(4, send5, recv5)

    gate_weights = halves(jnp.concatenate([weights_t[0, me], weights_t[1, me]], 0))
    gate_bias = jnp.concatenate([bias_t[0, me], bias_t[1, me]], 0)[:, :1]

    def keep_of(d):
        return jnp.concatenate(
            [blocks[d, cells + q : cells + q + 1, :] for q in range(cells // channels)], 1
        )

    def grads_of(offsets):
        devices = [me ^ t for t in offsets]

        def side_by_side(take):
            return jnp.concatenate([take(d) for d in devices], 1)

        x = halves(jnp.concatenate([blocks[d, :cells, :] for d in devices], 0))
        gates = jax.nn.sigmoid(dot_halves(gate_weights, x, NT) + gate_bias)
        values = side_by_side(lambda d: recv1[d])
        grads = side_by_side(lambda d: send5[d])
        present = side_by_side(keep_of)
        both = jnp.concatenate([grads * values * (1.0 - gates), grads * present * gates], 0)
        return dot_halves(halves(both), x, NN)

    def came_in(stage):
        return sorted({e[1] ^ e[2] for e in plan if e[0] == stage})

    first_ones = [0, *came_in(0), *came_in(1)]
    for block in first_ones:
        ensure(block)
    total = grads_of(first_ones)
    wait_for(recv_sems, 3, recv4.at[pl.ds(0, n // 2 - 1)])
    early[my_chip, my_core] = jnp.sum(recv4[...], 0) / length
    spread(5, early)
    gather(3)
    for stage in (2, 3):
        for block in came_in(stage):
            ensure(block)
        total = total + grads_of(came_in(stage))
    late[my_chip, my_core] = total / length
    spread(6, late)

    arrived(4, recv5)
    half = 2 * hidden
    d_left = merge_h(recv5[:, :own, :]) * keep_tall
    d_first = jnp.concatenate([d_left * p2 * p1 * (1.0 - p1), d_left * p1], 1)
    d_normed = d_normed + dot(d_first, win_ref[:, :half], NT)
    d_right = merge_h(recv5[:, own:, :]) * keep_tall
    d_second = jnp.concatenate([d_right * p4 * p3 * (1.0 - p3), d_right * p3], 1)
    d_normed = d_normed + dot(d_second, win_ref[:, half:width], NT)
    store_cells(gpair_ref, normalise_back(pair_hat, pair_scale, d_normed * gin_ref[...]))

    wait_for(recv_sems, 5, same_core(early))
    hand_over(7, early)
    wait_for(recv_sems, 6, same_core(late))
    hand_over(8, late)
    wait_for(recv_sems, 7, early.at[:, 0])
    gwin_ref[:, width:] = early[:, :, :own, :].reshape(channels, channels)
    gwout_ref[...] = early[:, :, own:, :].reshape(hidden, channels)
    wait_for(recv_sems, 8, late.at[:, 0])
    for q, k in enumerate((0, 2, 1, 3)):
        piece = late[:, :, q * own : (q + 1) * own, :].reshape(hidden, channels)
        gwin_ref[:, k * hidden : (k + 1) * hidden] = piece.T

    for phase, ref in ((0, recv1), (1, recv2), (2, recv3), (4, recv5)):
        sent(phase, ref)
    wait_for(send_sems, 3, recv4.at[pl.ds(0, n // 2 - 1)])
    wait_for(send_sems, 9, pair4)
    for phase, ref in ((5, early), (6, late)):
        wait_for(send_sems, phase, same_core(ref))
    for phase, ref in ((7, early), (8, late)):
        wait_for(send_sems, phase, ref.at[:, 0])
    for slot, (_, source, _, first, last) in enumerate(plan):
        wait_for(plan_send, slot, part_of(source, first, last))


def write_out(a, b, c, d, a_out, b_out, c_out, d_out, sems):
    pairs = ((a, a_out), (b, b_out), (c, c_out), (d, d_out))
    copies = [pltpu.make_async_copy(x, y, sems.at[k]) for k, (x, y) in enumerate(pairs)]
    for copy in copies:
        copy.start()
    for copy in copies:
        copy.wait()


def on_device(
    n_row,
    n_ch,
    pair_rep,
    pair_mask,
    ln_in_gain,
    ln_in_bias,
    w_in,
    b_in,
    ln_out_gain,
    ln_out_bias,
    w_out,
    b_out,
    cotangent,
):
    n = n_row * n_ch
    rows, length, channels = pair_rep.shape
    hidden = w_out.shape[0]
    own = hidden // n
    cells = rows * length
    f32 = jnp.float32

    def both(*shape):
        return [pltpu.VMEM((n, *shape), f32), pltpu.VMEM((n, *shape), f32)]

    inputs = (
        pair_rep,
        pair_mask,
        ln_in_gain[None],
        ln_in_bias[None],
        w_in,
        b_in.reshape(-1, min(128, hidden)),
        ln_out_gain[None],
        ln_out_bias[None],
        w_out,
        b_out[None],
        cotangent,
    )
    lanes = min(128, hidden)
    plan = gather_plan(n, n_ch, cells + 8)
    anywhere = pl.BlockSpec(memory_space=pl.ANY)
    vmem = pl.BlockSpec(memory_space=pltpu.VMEM)
    inputs = tuple(pltpu.with_memory_space_constraint(x, pltpu.MemorySpace.HBM) for x in inputs)
    out_shape = tuple(
        jax.ShapeDtypeStruct(x.shape, f32) for x in (pair_rep, pair_rep, w_in, w_out)
    )
    parts = pl.pallas_call(
        functools.partial(kernel, n_row, n_ch, plan),
        out_shape=out_shape,
        in_specs=[anywhere] * 11,
        out_specs=(vmem,) * 4,
        scratch_shapes=[
            *[pltpu.VMEM(x.shape, x.dtype) for x in inputs],
            *both(2 * own, cells),
            *both(own, cells),
            *both(own, cells),
            pltpu.VMEM((n // 2, 2, 2 * own, channels), f32),
            *[pltpu.VMEM((n // 2, 2 * own, channels), f32)] * 3,
            *both(2 * own, cells),
            pltpu.VMEM((n // 2, 2, 2 * own, channels), f32),
            pltpu.VMEM((n // 2, 2, 4 * own, channels), f32),
            pltpu.VMEM((n, cells + 8, channels), f32),
            pltpu.VMEM((2, n, own, channels), f32),
            pltpu.VMEM((2, n, own, lanes), f32),
            pltpu.SemaphoreType.DMA((10,)),
            pltpu.SemaphoreType.DMA((10,)),
            pltpu.SemaphoreType.DMA((len(plan),)),
            pltpu.SemaphoreType.DMA((len(plan),)),
            pltpu.SemaphoreType.DMA((11,)),
        ],
        compiler_params=pltpu.CompilerParams(
            collective_id=0, has_side_effects=True, vmem_limit_bytes=56 << 20
        ),
    )(*inputs)
    return pl.pallas_call(
        write_out,
        out_shape=out_shape,
        in_specs=[vmem] * 4,
        out_specs=(anywhere,) * 4,
        scratch_shapes=[pltpu.SemaphoreType.DMA((4,))],
        compiler_params=pltpu.CompilerParams(vmem_limit_bytes=8 << 20),
    )(*parts)


def solution(mesh):
    rows = P(("row", "ch"), None, None)
    placed = (rows, P(("row", "ch"), None), P(), P(), P(), P(), P(), P(), P(), P(), rows)
    return jax.shard_map(
        functools.partial(on_device, mesh.shape["row"], mesh.shape["ch"]),
        mesh=mesh,
        in_specs=placed,
        out_specs=(rows, rows, P(), P()),
        check_vma=False,
    )
```

```python
import functools

import jax
import jax.numpy as jnp
from jax import lax
from jax.experimental import pallas as pl
from jax.experimental.pallas import tpu as pltpu
from jax.sharding import PartitionSpec as P

epsilon = 1e-05
MESH = pl.DeviceIdType.MESH


def halves(a):
    high = a.astype(jnp.bfloat16)
    return high, (a - high.astype(jnp.float32)).astype(jnp.bfloat16)


def dot_halves(a, b, contract):
    def one(x, y):
        return lax.dot_general(
            x, y, (contract, ((), ())), preferred_element_type=jnp.float32
        )

    (a_high, a_low), (b_high, b_low) = a, b
    return one(a_high, b_low) + one(a_low, b_high) + one(a_high, b_high)


def dot(a, b, contract):
    return dot_halves(halves(a), halves(b), contract)


NN = ((1,), (0,))
NT = ((1,), (1,))
TN = ((0,), (0,))


def normalise(x):
    center = jnp.mean(x, -1, keepdims=True)
    spread = jnp.mean((x - center) ** 2, -1, keepdims=True)
    scale = lax.rsqrt(spread + epsilon)
    return (x - center) * scale, scale


def normalise_back(x_hat, scale, d_hat):
    return scale * (
        d_hat
        - jnp.mean(d_hat, -1, keepdims=True)
        - x_hat * jnp.mean(d_hat * x_hat, -1, keepdims=True)
    )


def farthest_first(n, n_ch):
    assert n & (n - 1) == 0

    def hops(t):
        row, ch = divmod(t, n_ch)
        return (row // 2).bit_length() + row % 2 + ch // 2

    return sorted(range(1, n), key=lambda t: (hops(t), t), reverse=True)


def gather_plan(n, n_ch, rows):
    core, side, up = 1, n_ch // 2, n_ch
    middle = rows // 16 * 8
    plan = []
    for z in range(0, n, 2 * n_ch):
        low = z & -z
        stage = 0 if z == 0 else 1 if z == low else 2
        if stage == 1:
            plan.append((0, 0, z, 0, rows))
        if stage == 2:
            near = z ^ low
            forwards = near & (near - 1) == 0
            plan.append((1, near, low, 0, rows) if forwards else (1, 0, z, 0, rows))
        plan.append((stage, z, side, 0, rows))
        plan.append((stage, z, up, 0, rows))
        if stage == 0:
            plan.append((0, 0, side ^ up, 0, rows))
        elif stage < 2:
            plan.append((stage + 1, z ^ side, up, 0, middle))
            plan.append((stage + 1, z ^ up, side, middle, rows))
        else:
            plan.append((1, 0, z ^ side ^ up, 0, rows))
        plan.append((stage, z, core, 0, rows))
        plan.append((stage + 1, z ^ side, core, 0, rows))
        plan.append((stage + 1, z ^ up, core, 0, rows))
        plan.append((1 if z == 0 else min(stage + 2, 3), z ^ side ^ up, core, 0, rows))
    return sorted(plan, key=lambda e: (e[0], e[2] == core))


def kernel(
    n_row,
    n_ch,
    plan,
    *refs,
):
    inputs, rest = refs[:11], refs[11:]
    update_ref, gpair_ref, gwin_ref, gwout_ref = rest[:4]
    held, rest = rest[4:15], rest[15:]
    (
        pair_ref,
        mask_ref,
        gin_ref,
        bin_ref,
        win_ref,
        b_ref,
        gout_ref,
        bout_ref,
        wout_ref,
        bo_ref,
        cot_ref,
    ) = held
    (
        send1,
        recv1,
        send2,
        recv2,
        send3,
        recv3,
        send4,
        pair4,
        sum4,
        recv4,
        send5,
        recv5,
        early,
        late,
        blocks,
        weights_t,
        bias_t,
        send_sems,
        recv_sems,
        plan_send,
        plan_recv,
        load_sems,
    ) = rest
    n = n_row * n_ch
    rows, length, channels = pair_ref.shape
    hidden = wout_ref.shape[0]
    own = hidden // n
    cells = rows * length
    my_row = lax.axis_index("row")
    my_ch = lax.axis_index("ch")
    me = my_row * n_ch + my_ch
    peers = farthest_first(n, n_ch)

    def place_of(t):
        d = me ^ t
        return d, (d // n_ch, lax.rem(d, n_ch))

    barrier = pltpu.get_barrier_semaphore()
    for t in peers:
        pl.semaphore_signal(barrier, inc=1, device_id=place_of(t)[1], device_id_type=MESH)

    loads = [
        pltpu.make_async_copy(inputs[k], held[k], load_sems.at[k]) for k in range(len(inputs))
    ]
    for k in (0, 2, 3, 4, 5, 1, 10, 6, 7, 8, 9):
        loads[k].start()

    def remote(phase, src, dst, to):
        pltpu.make_async_remote_copy(
            src_ref=src,
            dst_ref=dst,
            send_sem=send_sems.at[phase],
            recv_sem=recv_sems.at[phase],
            device_id=place_of(to)[1],
            device_id_type=MESH,
        ).start()

    def exchange(phase, src, dst):
        for t in peers:
            remote(phase, src.at[place_of(t)[0]], dst.at[me], t)
        dst[me] = src[me]

    def wait_for(sems, phase, ref):
        pltpu.make_async_copy(ref, ref, sems.at[phase]).wait()

    def arrived(phase, dst):
        wait_for(recv_sems, phase, dst.at[pl.ds(0, n - 1)])

    def sent(phase, dst):
        wait_for(send_sems, phase, dst.at[pl.ds(0, n - 1)])

    my_chip = me // 2
    my_core = lax.rem(me, 2)

    def spread(phase, ref):
        for t in peers:
            if t % 2 == 0:
                mine = ref.at[my_chip, my_core]
                remote(phase, mine, mine, t)

    def same_core(ref):
        return ref.at[pl.ds(0, n // 2 - 1), 0]

    def hand_over(phase, ref):
        mine = ref.at[:, my_core]
        remote(phase, mine, mine, 1)

    def part_of(held_by, first, last):
        return blocks.at[me ^ held_by, pl.ds(first, last - first)]

    here = {0}

    def ensure(block):
        if block in here:
            return
        here.add(block)
        for slot, (_, source, to, first, last) in enumerate(plan):
            if source ^ to == block:
                wait_for(plan_recv, slot, part_of(block, first, last))

    def gather(stage):
        for slot, (when, source, to, first, last) in enumerate(plan):
            if when == stage:
                ensure(source)
                part = part_of(source, first, last)
                pltpu.make_async_remote_copy(
                    src_ref=part,
                    dst_ref=part,
                    send_sem=plan_send.at[slot],
                    recv_sem=plan_recv.at[slot],
                    device_id=place_of(to)[1],
                    device_id_type=MESH,
                ).start()

    def load_cells(ref):
        return jnp.concatenate(
            [ref[i, pl.ds(p, n, stride=rows), :] for i in range(rows) for p in range(rows)], 0
        )

    def store_cells(ref, value):
        for i in range(rows):
            for p in range(rows):
                at = i * length + p * n
                ref[i, pl.ds(p, n, stride=rows), :] = value[at : at + n]

    def split_h(value):
        return value.T.reshape(n, own, cells)

    def merge_h(value):
        return value.reshape(hidden, cells).T

    def stack(value):
        return jnp.concatenate([value[:, i * length : (i + 1) * length] for i in range(rows)], 0)

    def unstack(value):
        return jnp.concatenate([value[i * n : (i + 1) * n] for i in range(rows)], 1)

    def bias(first, last):
        return jnp.concatenate([b_ref[k : k + 1] for k in range(first, last)], 1)

    natural = lax.broadcasted_iota(jnp.int32, (length, length), 0)
    place = lax.broadcasted_iota(jnp.int32, (length, length), 1)
    order = jnp.where(natural == lax.rem(place, n) * rows + place // n, 1.0, 0.0)
    loads[1].wait()
    keep = lax.dot_general(
        mask_ref[...].astype(jnp.bfloat16),
        order.astype(jnp.bfloat16),
        (NN, ((), ())),
        preferred_element_type=jnp.float32,
    )
    keep = jnp.concatenate([keep[i : i + 1] for i in range(rows)], 1)

    loads[0].wait()
    loads[2].wait()
    loads[3].wait()
    pair_hat, pair_scale = normalise(load_cells(pair_ref))
    normed = pair_hat * gin_ref[...] + bin_ref[...]
    width = 4 * hidden
    lanes = b_ref.shape[1]
    loads[4].wait()
    loads[5].wait()
    pieces = dot(normed, win_ref[:, :width], NN) + bias(0, width // lanes)
    p1 = jax.nn.sigmoid(pieces[:, :hidden])
    p2 = pieces[:, hidden : 2 * hidden]
    p3 = jax.nn.sigmoid(pieces[:, 2 * hidden : 3 * hidden])
    p4 = pieces[:, 3 * hidden :]
    keep_tall = jnp.broadcast_to(keep, (hidden, cells)).T
    left = keep_tall * p1 * p2
    right = keep_tall * p3 * p4
    send1[:, :own, :] = split_h(left)
    send1[:, own:, :] = split_h(right)
    blocks[me, :cells, :] = normed
    for q in range(8):
        at = min(q, cells // channels - 1) * channels
        blocks[me, cells + q : cells + q + 1, :] = keep[:, at : at + channels]
    pl.semaphore_wait(barrier, n - 1)
    exchange(0, send1, recv1)
    gather(0)

    for q, k in enumerate((0, 2)):
        at = k * hidden
        weights_t[q] = win_ref[:, at : at + hidden].T.reshape(n, own, channels)
        column = b_ref[at // lanes : at // lanes + 1]
        bias_t[q] = jnp.broadcast_to(column, (lanes, hidden)).T.reshape(n, own, lanes)

    gate = jax.nn.sigmoid(dot(normed, win_ref[:, width:], NN) + bias(width // lanes, b_ref.shape[0]))
    for k in range(6, 11):
        loads[k].wait()
    cot = load_cells(cot_ref)

    arrived(0, recv1)
    lefts = [stack(recv1[:, h, :]) for h in range(own)]
    rights = [stack(recv1[:, own + h, :]) for h in range(own)]
    for h in range(own):
        send2[:, h, :] = unstack(dot(lefts[h], rights[h], NT))
    exchange(1, send2, recv2)
    gather(1)
    arrived(1, recv2)

    prod_hat, prod_scale = normalise(merge_h(recv2[...]))
    normed_product = prod_hat * gout_ref[...] + bout_ref[...]
    projected = dot(normed_product, wout_ref[...], NN) + bo_ref[...]
    d_out = cot * gate
    d_product = normalise_back(
        prod_hat, prod_scale, dot(d_out, wout_ref[...], NT) * gout_ref[...]
    )
    send3[...] = split_h(d_product)
    exchange(2, send3, recv3)

    store_cells(update_ref, gate * projected)
    d_gate = cot * projected * gate * (1.0 - gate)
    d_wout = dot(normed_product, d_out, TN)
    d_wgate = dot(normed, d_gate, TN)
    send4[:, :, :own, :] = d_wgate.reshape(n // 2, 2, own, channels)
    send4[:, :, own:, :] = d_wout.reshape(n // 2, 2, own, channels)
    remote(9, send4.at[:, 1 - my_core], pair4, 1)
    gather(2)
    d_normed = dot(d_gate, win_ref[:, width:], NT)
    wait_for(recv_sems, 9, pair4)
    sum4[...] = send4[:, my_core] + pair4[...]
    for t in peers:
        if t % 2 == 0:
            remote(3, sum4.at[place_of(t)[0] // 2], recv4.at[my_chip], t)
    recv4[my_chip] = sum4[my_chip]

    arrived(2, recv3)
    d_cols = [stack(recv3[:, h, :]) for h in range(own)]
    for h in range(own):
        send5[:, h, :] = unstack(dot(d_cols[h], rights[h], NN))
    for h in range(own):
        send5[:, own + h, :] = unstack(dot(d_cols[h], lefts[h], TN))
    exchange(4, send5, recv5)

    gate_weights = halves(jnp.concatenate([weights_t[0, me], weights_t[1, me]], 0))
    gate_bias = jnp.concatenate([bias_t[0, me], bias_t[1, me]], 0)[:, :1]

    def keep_of(d):
        return jnp.concatenate(
            [blocks[d, cells + q : cells + q + 1, :] for q in range(cells // channels)], 1
        )

    def grads_of(offsets):
        devices = [me ^ t for t in offsets]

        def side_by_side(take):
            return jnp.concatenate([take(d) for d in devices], 1)

        x = halves(jnp.concatenate([blocks[d, :cells, :] for d in devices], 0))
        gates = jax.nn.sigmoid(dot_halves(gate_weights, x, NT) + gate_bias)
        values = side_by_side(lambda d: recv1[d])
        grads = side_by_side(lambda d: send5[d])
        present = side_by_side(keep_of)
        both = jnp.concatenate([grads * values * (1.0 - gates), grads * present * gates], 0)
        return dot_halves(halves(both), x, NN)

    def came_in(stage):
        return sorted({e[1] ^ e[2] for e in plan if e[0] == stage})

    first_ones = [0, *came_in(0), *came_in(1)]
    for block in first_ones:
        ensure(block)
    total = grads_of(first_ones)
    wait_for(recv_sems, 3, recv4.at[pl.ds(0, n // 2 - 1)])
    early[my_chip, my_core] = jnp.sum(recv4[...], 0) / length
    spread(5, early)
    gather(3)
    for stage in (2, 3):
        for block in came_in(stage):
            ensure(block)
        total = total + grads_of(came_in(stage))
    late[my_chip, my_core] = total / length
    spread(6, late)

    arrived(4, recv5)
    half = 2 * hidden
    d_left = merge_h(recv5[:, :own, :]) * keep_tall
    d_first = jnp.concatenate([d_left * p2 * p1 * (1.0 - p1), d_left * p1], 1)
    d_normed = d_normed + dot(d_first, win_ref[:, :half], NT)
    d_right = merge_h(recv5[:, own:, :]) * keep_tall
    d_second = jnp.concatenate([d_right * p4 * p3 * (1.0 - p3), d_right * p3], 1)
    d_normed = d_normed + dot(d_second, win_ref[:, half:width], NT)
    store_cells(gpair_ref, normalise_back(pair_hat, pair_scale, d_normed * gin_ref[...]))

    wait_for(recv_sems, 5, same_core(early))
    hand_over(7, early)
    wait_for(recv_sems, 6, same_core(late))
    hand_over(8, late)
    wait_for(recv_sems, 7, early.at[:, 0])
    gwin_ref[:, width:] = early[:, :, :own, :].reshape(channels, channels)
    gwout_ref[...] = early[:, :, own:, :].reshape(hidden, channels)
    wait_for(recv_sems, 8, late.at[:, 0])
    for q, k in enumerate((0, 2, 1, 3)):
        piece = late[:, :, q * own : (q + 1) * own, :].reshape(hidden, channels)
        gwin_ref[:, k * hidden : (k + 1) * hidden] = piece.T

    for phase, ref in ((0, recv1), (1, recv2), (2, recv3), (4, recv5)):
        sent(phase, ref)
    wait_for(send_sems, 3, recv4.at[pl.ds(0, n // 2 - 1)])
    wait_for(send_sems, 9, pair4)
    for phase, ref in ((5, early), (6, late)):
        wait_for(send_sems, phase, same_core(ref))
    for phase, ref in ((7, early), (8, late)):
        wait_for(send_sems, phase, ref.at[:, 0])
    for slot, (_, source, _, first, last) in enumerate(plan):
        wait_for(plan_send, slot, part_of(source, first, last))


def write_out(a, b, c, d, a_out, b_out, c_out, d_out, sems):
    pairs = ((a, a_out), (b, b_out), (c, c_out), (d, d_out))
    copies = [pltpu.make_async_copy(x, y, sems.at[k]) for k, (x, y) in enumerate(pairs)]
    for copy in copies:
        copy.start()
    for copy in copies:
        copy.wait()


def on_device(
    n_row,
    n_ch,
    pair_rep,
    pair_mask,
    ln_in_gain,
    ln_in_bias,
    w_in,
    b_in,
    ln_out_gain,
    ln_out_bias,
    w_out,
    b_out,
    cotangent,
):
    n = n_row * n_ch
    rows, length, channels = pair_rep.shape
    hidden = w_out.shape[0]
    own = hidden // n
    cells = rows * length
    f32 = jnp.float32

    def both(*shape):
        return [pltpu.VMEM((n, *shape), f32), pltpu.VMEM((n, *shape), f32)]

    inputs = (
        pair_rep,
        pair_mask,
        ln_in_gain[None],
        ln_in_bias[None],
        w_in,
        b_in.reshape(-1, min(128, hidden)),
        ln_out_gain[None],
        ln_out_bias[None],
        w_out,
        b_out[None],
        cotangent,
    )
    lanes = min(128, hidden)
    plan = gather_plan(n, n_ch, cells + 8)
    anywhere = pl.BlockSpec(memory_space=pl.ANY)
    vmem = pl.BlockSpec(memory_space=pltpu.VMEM)
    inputs = tuple(pltpu.with_memory_space_constraint(x, pltpu.MemorySpace.HBM) for x in inputs)
    out_shape = tuple(
        jax.ShapeDtypeStruct(x.shape, f32) for x in (pair_rep, pair_rep, w_in, w_out)
    )
    parts = pl.pallas_call(
        functools.partial(kernel, n_row, n_ch, plan),
        out_shape=out_shape,
        in_specs=[anywhere] * 11,
        out_specs=(vmem,) * 4,
        scratch_shapes=[
            *[pltpu.VMEM(x.shape, x.dtype) for x in inputs],
            *both(2 * own, cells),
            *both(own, cells),
            *both(own, cells),
            pltpu.VMEM((n // 2, 2, 2 * own, channels), f32),
            *[pltpu.VMEM((n // 2, 2 * own, channels), f32)] * 3,
            *both(2 * own, cells),
            pltpu.VMEM((n // 2, 2, 2 * own, channels), f32),
            pltpu.VMEM((n // 2, 2, 4 * own, channels), f32),
            pltpu.VMEM((n, cells + 8, channels), f32),
            pltpu.VMEM((2, n, own, channels), f32),
            pltpu.VMEM((2, n, own, lanes), f32),
            pltpu.SemaphoreType.DMA((10,)),
            pltpu.SemaphoreType.DMA((10,)),
            pltpu.SemaphoreType.DMA((len(plan),)),
            pltpu.SemaphoreType.DMA((len(plan),)),
            pltpu.SemaphoreType.DMA((11,)),
        ],
        compiler_params=pltpu.CompilerParams(
            collective_id=0,
            has_side_effects=True,
            vmem_limit_bytes=n * (cells + 8) * channels * 4 + (22 << 20),
        ),
    )(*inputs)
    return pl.pallas_call(
        write_out,
        out_shape=out_shape,
        in_specs=[vmem] * 4,
        out_specs=(anywhere,) * 4,
        scratch_shapes=[pltpu.SemaphoreType.DMA((4,))],
        compiler_params=pltpu.CompilerParams(vmem_limit_bytes=8 << 20),
    )(*parts)


def solution(mesh):
    rows = P(("row", "ch"), None, None)
    placed = (rows, P(("row", "ch"), None), P(), P(), P(), P(), P(), P(), P(), P(), rows)
    return jax.shard_map(
        functools.partial(on_device, mesh.shape["row"], mesh.shape["ch"]),
        mesh=mesh,
        in_specs=placed,
        out_specs=(rows, rows, P(), P()),
        check_vma=False,
    )
```

```python
import functools

import jax
import jax.numpy as jnp
from jax import lax
from jax.experimental import pallas as pl
from jax.experimental.pallas import tpu as pltpu
from jax.sharding import PartitionSpec as P

epsilon = 1e-05
MESH = pl.DeviceIdType.MESH


def halves(a):
    high = a.astype(jnp.bfloat16)
    return high, (a - high.astype(jnp.float32)).astype(jnp.bfloat16)


def dot_halves(a, b, contract):
    def one(x, y):
        return lax.dot_general(
            x, y, (contract, ((), ())), preferred_element_type=jnp.float32
        )

    (a_high, a_low), (b_high, b_low) = a, b
    return one(a_high, b_low) + one(a_low, b_high) + one(a_high, b_high)


def dot(a, b, contract):
    return dot_halves(halves(a), halves(b), contract)


NN = ((1,), (0,))
NT = ((1,), (1,))
TN = ((0,), (0,))


def normalise(x):
    center = jnp.mean(x, -1, keepdims=True)
    spread = jnp.mean((x - center) ** 2, -1, keepdims=True)
    scale = lax.rsqrt(spread + epsilon)
    return (x - center) * scale, scale


def normalise_back(x_hat, scale, d_hat):
    return scale * (
        d_hat
        - jnp.mean(d_hat, -1, keepdims=True)
        - x_hat * jnp.mean(d_hat * x_hat, -1, keepdims=True)
    )


def farthest_first(n, n_ch):
    assert n & (n - 1) == 0

    def hops(t):
        row, ch = divmod(t, n_ch)
        return (row // 2).bit_length() + row % 2 + ch // 2

    return sorted(range(1, n), key=lambda t: (hops(t), t), reverse=True)


def gather_plan(n, n_ch, rows):
    core, side, up = 1, n_ch // 2, n_ch
    middle = rows // 16 * 8
    plan = []
    for z in range(0, n, 2 * n_ch):
        low = z & -z
        stage = 0 if z == 0 else 1 if z == low else 2
        if stage == 1:
            plan.append((0, 0, z, 0, rows))
        if stage == 2:
            near = z ^ low
            forwards = near & (near - 1) == 0
            plan.append((1, near, low, 0, rows) if forwards else (1, 0, z, 0, rows))
        plan.append((stage, z, side, 0, rows))
        plan.append((stage, z, up, 0, rows))
        if stage == 0:
            plan.append((0, 0, side ^ up, 0, rows))
        elif stage < 2:
            plan.append((stage + 1, z ^ side, up, 0, middle))
            plan.append((stage + 1, z ^ up, side, middle, rows))
        else:
            plan.append((1, side ^ up, z, 0, rows))
        plan.append((stage, z, core, 0, rows))
        plan.append((stage + 1, z ^ side, core, 0, rows))
        plan.append((stage + 1, z ^ up, core, 0, rows))
        plan.append((1 if z == 0 else min(stage + 2, 3), z ^ side ^ up, core, 0, rows))
    return sorted(plan, key=lambda e: (e[0], e[2] == core, e[1] > 2 * n_ch and e[2] < 2 * n_ch))


def kernel(
    n_row,
    n_ch,
    plan,
    *refs,
):
    inputs, rest = refs[:11], refs[11:]
    update_ref, gpair_ref, gwin_ref, gwout_ref = rest[:4]
    held, rest = rest[4:15], rest[15:]
    (
        pair_ref,
        mask_ref,
        gin_ref,
        bin_ref,
        win_ref,
        b_ref,
        gout_ref,
        bout_ref,
        wout_ref,
        bo_ref,
        cot_ref,
    ) = held
    (
        send1,
        recv1,
        send2,
        recv2,
        send3,
        recv3,
        send4,
        pair4,
        sum4,
        recv4,
        send5,
        recv5,
        early,
        late,
        factors,
        blocks,
        weights_t,
        bias_t,
        send_sems,
        recv_sems,
        plan_send,
        plan_recv,
        load_sems,
    ) = rest
    n = n_row * n_ch
    rows, length, channels = pair_ref.shape
    hidden = wout_ref.shape[0]
    own = hidden // n
    cells = rows * length
    my_row = lax.axis_index("row")
    my_ch = lax.axis_index("ch")
    me = my_row * n_ch + my_ch
    peers = farthest_first(n, n_ch)

    def place_of(t):
        d = me ^ t
        return d, (d // n_ch, lax.rem(d, n_ch))

    barrier = pltpu.get_barrier_semaphore()
    for t in peers:
        pl.semaphore_signal(barrier, inc=1, device_id=place_of(t)[1], device_id_type=MESH)

    loads = [
        pltpu.make_async_copy(inputs[k], held[k], load_sems.at[k]) for k in range(len(inputs))
    ]
    for k in (0, 2, 3, 4, 5, 1, 10, 6, 7, 8, 9):
        loads[k].start()

    def remote(phase, src, dst, to):
        pltpu.make_async_remote_copy(
            src_ref=src,
            dst_ref=dst,
            send_sem=send_sems.at[phase],
            recv_sem=recv_sems.at[phase],
            device_id=place_of(to)[1],
            device_id_type=MESH,
        ).start()

    def exchange(phase, src, dst):
        for t in peers:
            remote(phase, src.at[place_of(t)[0]], dst.at[me], t)
        dst[me] = src[me]

    def wait_for(sems, phase, ref):
        pltpu.make_async_copy(ref, ref, sems.at[phase]).wait()

    def arrived(phase, dst):
        wait_for(recv_sems, phase, dst.at[pl.ds(0, n - 1)])

    def sent(phase, dst):
        wait_for(send_sems, phase, dst.at[pl.ds(0, n - 1)])

    my_chip = me // 2
    my_core = lax.rem(me, 2)

    def spread(phase, ref):
        for t in peers:
            if t % 2 == 0:
                mine = ref.at[my_chip, my_core]
                remote(phase, mine, mine, t)

    def same_core(ref):
        return ref.at[pl.ds(0, n // 2 - 1), 0]

    def hand_over(phase, ref):
        mine = ref.at[:, my_core]
        remote(phase, mine, mine, 1)

    def part_of(held_by, first, last):
        return blocks.at[me ^ held_by, pl.ds(first, last - first)]

    here = {0}

    def ensure(block):
        if block in here:
            return
        here.add(block)
        for slot, (_, source, to, first, last) in enumerate(plan):
            if source ^ to == block:
                wait_for(plan_recv, slot, part_of(block, first, last))

    def gather(stage):
        for slot, (when, source, to, first, last) in enumerate(plan):
            if when == stage:
                ensure(source)
                part = part_of(source, first, last)
                pltpu.make_async_remote_copy(
                    src_ref=part,
                    dst_ref=part,
                    send_sem=plan_send.at[slot],
                    recv_sem=plan_recv.at[slot],
                    device_id=place_of(to)[1],
                    device_id_type=MESH,
                ).start()

    def load_cells(ref):
        return jnp.concatenate(
            [ref[i, pl.ds(p, n, stride=rows), :] for i in range(rows) for p in range(rows)], 0
        )

    def store_cells(ref, value):
        for i in range(rows):
            for p in range(rows):
                at = i * length + p * n
                ref[i, pl.ds(p, n, stride=rows), :] = value[at : at + n]

    def split_h(value):
        return value.T.reshape(n, own, cells)

    def merge_h(value):
        return value.reshape(hidden, cells).T

    def stack(value):
        return jnp.concatenate([value[:, i * length : (i + 1) * length] for i in range(rows)], 0)

    def unstack(value):
        return jnp.concatenate([value[i * n : (i + 1) * n] for i in range(rows)], 1)

    def bias(first, last):
        return jnp.concatenate([b_ref[k : k + 1] for k in range(first, last)], 1)

    natural = lax.broadcasted_iota(jnp.int32, (length, length), 0)
    place = lax.broadcasted_iota(jnp.int32, (length, length), 1)
    order = jnp.where(natural == lax.rem(place, n) * rows + place // n, 1.0, 0.0)
    loads[1].wait()
    keep = lax.dot_general(
        mask_ref[...].astype(jnp.bfloat16),
        order.astype(jnp.bfloat16),
        (NN, ((), ())),
        preferred_element_type=jnp.float32,
    )
    keep = jnp.concatenate([keep[i : i + 1] for i in range(rows)], 1)

    loads[0].wait()
    loads[2].wait()
    loads[3].wait()
    pair_hat, pair_scale = normalise(load_cells(pair_ref))
    normed = pair_hat * gin_ref[...] + bin_ref[...]
    width = 4 * hidden
    lanes = b_ref.shape[1]
    loads[4].wait()
    loads[5].wait()
    pieces = dot(normed, win_ref[:, :width], NN) + bias(0, width // lanes)
    p1 = jax.nn.sigmoid(pieces[:, :hidden])
    p2 = pieces[:, hidden : 2 * hidden]
    p3 = jax.nn.sigmoid(pieces[:, 2 * hidden : 3 * hidden])
    p4 = pieces[:, 3 * hidden :]
    keep_tall = jnp.broadcast_to(keep, (hidden, cells)).T
    left = keep_tall * p1 * p2
    right = keep_tall * p3 * p4
    send1[:, :own, :] = split_h(left)
    send1[:, own:, :] = split_h(right)
    blocks[me, :cells, :] = normed
    for q in range(8):
        at = min(q, cells // channels - 1) * channels
        blocks[me, cells + q : cells + q + 1, :] = keep[:, at : at + channels]
    pl.semaphore_wait(barrier, n - 1)
    exchange(0, send1, recv1)
    gather(0)

    for q, k in enumerate((0, 2)):
        at = k * hidden
        weights_t[q] = win_ref[:, at : at + hidden].T.reshape(n, own, channels)
        column = b_ref[at // lanes : at // lanes + 1]
        bias_t[q] = jnp.broadcast_to(column, (lanes, hidden)).T.reshape(n, own, lanes)

    gate = jax.nn.sigmoid(dot(normed, win_ref[:, width:], NN) + bias(width // lanes, b_ref.shape[0]))
    for k in range(6, 11):
        loads[k].wait()
    cot = load_cells(cot_ref)

    arrived(0, recv1)
    lefts = [stack(recv1[:, h, :]) for h in range(own)]
    rights = [stack(recv1[:, own + h, :]) for h in range(own)]
    for h in range(own):
        send2[:, h, :] = unstack(dot(lefts[h], rights[h], NT))
    exchange(1, send2, recv2)
    gather(1)
    arrived(1, recv2)

    prod_hat, prod_scale = normalise(merge_h(recv2[...]))
    normed_product = prod_hat * gout_ref[...] + bout_ref[...]
    projected = dot(normed_product, wout_ref[...], NN) + bo_ref[...]
    d_out = cot * gate
    d_product = normalise_back(
        prod_hat, prod_scale, dot(d_out, wout_ref[...], NT) * gout_ref[...]
    )
    send3[...] = split_h(d_product)
    exchange(2, send3, recv3)
    gather(2)

    store_cells(update_ref, gate * projected)
    d_gate = cot * projected * gate * (1.0 - gate)
    d_wout = dot(normed_product, d_out, TN)
    d_wgate = dot(normed, d_gate, TN)
    send4[:, :, :own, :] = d_wgate.reshape(n // 2, 2, own, channels)
    send4[:, :, own:, :] = d_wout.reshape(n // 2, 2, own, channels)
    remote(7, send4.at[:, 1 - my_core], pair4, 1)
    d_normed = dot(d_gate, win_ref[:, width:], NT)
    wait_for(recv_sems, 7, pair4)
    sum4[...] = send4[:, my_core] + pair4[...]
    for t in peers:
        if t % 2 == 0:
            remote(3, sum4.at[place_of(t)[0] // 2], recv4.at[my_chip], t)
    recv4[my_chip] = sum4[my_chip]

    gate_weights = halves(jnp.concatenate([weights_t[0, me], weights_t[1, me]], 0))
    gate_bias = jnp.concatenate([bias_t[0, me], bias_t[1, me]], 0)[:, :1]

    def keep_of(d):
        return jnp.concatenate(
            [blocks[d, cells + q : cells + q + 1, :] for q in range(cells // channels)], 1
        )

    def side_by_side(take, offsets):
        return jnp.concatenate([take(me ^ t) for t in offsets], 1)

    def block_halves(offsets):
        return halves(jnp.concatenate([blocks[me ^ t, :cells, :] for t in offsets], 0))

    def factors_of(offsets, x):
        gates = jax.nn.sigmoid(dot_halves(gate_weights, x, NT) + gate_bias)
        values = side_by_side(lambda d: recv1[d], offsets)
        present = side_by_side(keep_of, offsets)
        return jnp.concatenate([values * (1.0 - gates), present * gates], 0)

    def grads_of(offsets, x, scaled):
        grads = side_by_side(lambda d: send5[d], offsets)
        return dot_halves(halves(jnp.concatenate([grads, grads], 0) * scaled), x, NN)

    def came_in(stage):
        return sorted({e[1] ^ e[2] for e in plan if e[0] == stage})

    first_ones = [0, *came_in(0), *came_in(1)]
    for block in first_ones:
        ensure(block)
    first_factors = factors_of(first_ones, block_halves(first_ones))
    for at, t in enumerate(first_ones):
        factors[me ^ t] = first_factors[:, at * cells : (at + 1) * cells]

    arrived(2, recv3)
    d_cols = [stack(recv3[:, h, :]) for h in range(own)]
    for h in range(own):
        send5[:, h, :] = unstack(dot(d_cols[h], rights[h], NN))
    for h in range(own):
        send5[:, own + h, :] = unstack(dot(d_cols[h], lefts[h], TN))
    exchange(4, send5, recv5)
    gather(3)
    total = grads_of(
        first_ones, block_halves(first_ones), side_by_side(lambda d: factors[d], first_ones)
    )
    wait_for(recv_sems, 3, recv4.at[pl.ds(0, n // 2 - 1)])
    early[my_chip, my_core] = jnp.sum(recv4[...], 0) / length
    spread(8, early)
    for stage in (2, 3):
        for block in came_in(stage):
            ensure(block)
        x = block_halves(came_in(stage))
        total = total + grads_of(came_in(stage), x, factors_of(came_in(stage), x))
    late[my_chip, my_core] = total / length
    spread(5, late)

    arrived(4, recv5)
    half = 2 * hidden
    d_left = merge_h(recv5[:, :own, :]) * keep_tall
    d_first = jnp.concatenate([d_left * p2 * p1 * (1.0 - p1), d_left * p1], 1)
    d_normed = d_normed + dot(d_first, win_ref[:, :half], NT)
    d_right = merge_h(recv5[:, own:, :]) * keep_tall
    d_second = jnp.concatenate([d_right * p4 * p3 * (1.0 - p3), d_right * p3], 1)
    d_normed = d_normed + dot(d_second, win_ref[:, half:width], NT)
    store_cells(gpair_ref, normalise_back(pair_hat, pair_scale, d_normed * gin_ref[...]))

    wait_for(recv_sems, 8, same_core(early))
    hand_over(9, early)
    for phase, ref in ((0, recv1), (1, recv2), (2, recv3), (4, recv5)):
        sent(phase, ref)
    wait_for(send_sems, 3, recv4.at[pl.ds(0, n // 2 - 1)])
    wait_for(send_sems, 7, pair4)
    for slot, (_, source, _, first, last) in enumerate(plan):
        wait_for(plan_send, slot, part_of(source, first, last))
    wait_for(send_sems, 8, same_core(early))
    wait_for(recv_sems, 5, same_core(late))
    hand_over(6, late)
    wait_for(recv_sems, 9, early.at[:, 0])
    gwin_ref[:, width:] = early[:, :, :own, :].reshape(channels, channels)
    gwout_ref[...] = early[:, :, own:, :].reshape(hidden, channels)
    wait_for(recv_sems, 6, late.at[:, 0])
    for q, k in enumerate((0, 2, 1, 3)):
        piece = late[:, :, q * own : (q + 1) * own, :].reshape(hidden, channels)
        gwin_ref[:, k * hidden : (k + 1) * hidden] = piece.T

    wait_for(send_sems, 5, same_core(late))
    for phase, ref in ((9, early), (6, late)):
        wait_for(send_sems, phase, ref.at[:, 0])


def write_out(a, b, c, d, a_out, b_out, c_out, d_out, sems):
    pairs = ((a, a_out), (b, b_out), (c, c_out), (d, d_out))
    copies = [pltpu.make_async_copy(x, y, sems.at[k]) for k, (x, y) in enumerate(pairs)]
    for copy in copies:
        copy.start()
    for copy in copies:
        copy.wait()


def on_device(
    n_row,
    n_ch,
    pair_rep,
    pair_mask,
    ln_in_gain,
    ln_in_bias,
    w_in,
    b_in,
    ln_out_gain,
    ln_out_bias,
    w_out,
    b_out,
    cotangent,
):
    n = n_row * n_ch
    rows, length, channels = pair_rep.shape
    hidden = w_out.shape[0]
    own = hidden // n
    cells = rows * length
    f32 = jnp.float32

    def both(*shape):
        return [pltpu.VMEM((n, *shape), f32), pltpu.VMEM((n, *shape), f32)]

    inputs = (
        pair_rep,
        pair_mask,
        ln_in_gain[None],
        ln_in_bias[None],
        w_in,
        b_in.reshape(-1, min(128, hidden)),
        ln_out_gain[None],
        ln_out_bias[None],
        w_out,
        b_out[None],
        cotangent,
    )
    lanes = min(128, hidden)
    plan = gather_plan(n, n_ch, cells + 8)
    anywhere = pl.BlockSpec(memory_space=pl.ANY)
    vmem = pl.BlockSpec(memory_space=pltpu.VMEM)
    inputs = tuple(pltpu.with_memory_space_constraint(x, pltpu.MemorySpace.HBM) for x in inputs)
    out_shape = tuple(
        jax.ShapeDtypeStruct(x.shape, f32) for x in (pair_rep, pair_rep, w_in, w_out)
    )
    parts = pl.pallas_call(
        functools.partial(kernel, n_row, n_ch, plan),
        out_shape=out_shape,
        in_specs=[anywhere] * 11,
        out_specs=(vmem,) * 4,
        scratch_shapes=[
            *[pltpu.VMEM(x.shape, x.dtype) for x in inputs],
            *both(2 * own, cells),
            *both(own, cells),
            *both(own, cells),
            pltpu.VMEM((n // 2, 2, 2 * own, channels), f32),
            *[pltpu.VMEM((n // 2, 2 * own, channels), f32)] * 3,
            *both(2 * own, cells),
            pltpu.VMEM((n // 2, 2, 2 * own, channels), f32),
            pltpu.VMEM((n // 2, 2, 4 * own, channels), f32),
            pltpu.VMEM((n, 4 * own, cells), f32),
            pltpu.VMEM((n, cells + 8, channels), f32),
            pltpu.VMEM((2, n, own, channels), f32),
            pltpu.VMEM((2, n, own, lanes), f32),
            pltpu.SemaphoreType.DMA((10,)),
            pltpu.SemaphoreType.DMA((10,)),
            pltpu.SemaphoreType.DMA((len(plan),)),
            pltpu.SemaphoreType.DMA((len(plan),)),
            pltpu.SemaphoreType.DMA((11,)),
        ],
        compiler_params=pltpu.CompilerParams(
            collective_id=0,
            has_side_effects=True,
            vmem_limit_bytes=n * (cells + 8) * channels * 4 + (22 << 20),
        ),
    )(*inputs)
    return pl.pallas_call(
        write_out,
        out_shape=out_shape,
        in_specs=[vmem] * 4,
        out_specs=(anywhere,) * 4,
        scratch_shapes=[pltpu.SemaphoreType.DMA((4,))],
        compiler_params=pltpu.CompilerParams(vmem_limit_bytes=8 << 20),
    )(*parts)


def solution(mesh):
    rows = P(("row", "ch"), None, None)
    placed = (rows, P(("row", "ch"), None), P(), P(), P(), P(), P(), P(), P(), P(), rows)
    return jax.shard_map(
        functools.partial(on_device, mesh.shape["row"], mesh.shape["ch"]),
        mesh=mesh,
        in_specs=placed,
        out_specs=(rows, rows, P(), P()),
        check_vma=False,
    )
```

```python
import functools

import jax
import jax.numpy as jnp
from jax import lax
from jax.experimental import pallas as pl
from jax.experimental.pallas import tpu as pltpu
from jax.sharding import PartitionSpec as P

epsilon = 1e-05
MESH = pl.DeviceIdType.MESH


def halves(a):
    high = a.astype(jnp.bfloat16)
    return high, (a - high.astype(jnp.float32)).astype(jnp.bfloat16)


def dot_halves(a, b, contract):
    def one(x, y):
        return lax.dot_general(
            x, y, (contract, ((), ())), preferred_element_type=jnp.float32
        )

    (a_high, a_low), (b_high, b_low) = a, b
    return one(a_high, b_low) + one(a_low, b_high) + one(a_high, b_high)


def dot(a, b, contract):
    return dot_halves(halves(a), halves(b), contract)


NN = ((1,), (0,))
NT = ((1,), (1,))
TN = ((0,), (0,))


def normalise(x):
    center = jnp.mean(x, -1, keepdims=True)
    spread = jnp.mean((x - center) ** 2, -1, keepdims=True)
    scale = lax.rsqrt(spread + epsilon)
    return (x - center) * scale, scale


def normalise_back(x_hat, scale, d_hat):
    return scale * (
        d_hat
        - jnp.mean(d_hat, -1, keepdims=True)
        - x_hat * jnp.mean(d_hat * x_hat, -1, keepdims=True)
    )


def farthest_first(n, n_ch):
    assert n & (n - 1) == 0

    def hops(t):
        row, ch = divmod(t, n_ch)
        return (row // 2).bit_length() + row % 2 + ch // 2

    return sorted(range(1, n), key=lambda t: (-hops(t), t % 2, t))


def gather_plan(n, n_ch, rows):
    core, side, up = 1, n_ch // 2, n_ch
    middle = rows // 16 * 8
    plan = []
    for z in range(0, n, 2 * n_ch):
        low = z & -z
        stage = 0 if z == 0 else 1 if z == low else 2
        if stage == 1:
            plan.append((0, 0, z, 0, rows))
        if stage == 2:
            near = z ^ low
            forwards = near & (near - 1) == 0
            plan.append((1, near, low, 0, rows) if forwards else (1, 0, z, 0, rows))
        plan.append((stage, z, side, 0, rows))
        plan.append((stage, z, up, 0, rows))
        if stage == 0:
            plan.append((0, 0, side ^ up, 0, rows))
        elif stage < 2:
            plan.append((stage + 1, z ^ side, up, 0, middle))
            plan.append((stage + 1, z ^ up, side, middle, rows))
        else:
            plan.append((1, side ^ up, z, 0, rows))
        plan.append((stage, z, core, 0, rows))
        plan.append((stage + 1, z ^ side, core, 0, rows))
        plan.append((stage + 1, z ^ up, core, 0, rows))
        plan.append((1 if z == 0 else min(stage + 2, 3), z ^ side ^ up, core, 0, rows))
    return sorted(plan, key=lambda e: (e[0], e[2] == core, e[1] > 2 * n_ch and e[2] < 2 * n_ch))


def kernel(
    n_row,
    n_ch,
    plan,
    *refs,
):
    inputs, rest = refs[:11], refs[11:]
    update_ref, gpair_ref, gwin_ref, gwout_ref = rest[:4]
    held, rest = rest[4:15], rest[15:]
    (
        pair_ref,
        mask_ref,
        gin_ref,
        bin_ref,
        win_ref,
        b_ref,
        gout_ref,
        bout_ref,
        wout_ref,
        bo_ref,
        cot_ref,
    ) = held
    (
        send1,
        recv1,
        send2,
        recv2,
        send3,
        recv3,
        send4,
        pair4,
        sum4,
        recv4,
        send5,
        recv5,
        early,
        late,
        factors,
        blocks,
        weights_t,
        bias_t,
        send_sems,
        recv_sems,
        plan_send,
        plan_recv,
        load_sems,
    ) = rest
    n = n_row * n_ch
    rows, length, channels = pair_ref.shape
    hidden = wout_ref.shape[0]
    own = hidden // n
    cells = rows * length
    my_row = lax.axis_index("row")
    my_ch = lax.axis_index("ch")
    me = my_row * n_ch + my_ch
    peers = farthest_first(n, n_ch)

    def place_of(t):
        d = me ^ t
        return d, (d // n_ch, lax.rem(d, n_ch))

    barrier = pltpu.get_barrier_semaphore()
    for t in peers:
        pl.semaphore_signal(barrier, inc=1, device_id=place_of(t)[1], device_id_type=MESH)

    loads = [
        pltpu.make_async_copy(inputs[k], held[k], load_sems.at[k]) for k in range(len(inputs))
    ]
    for k in (0, 2, 3, 4, 5, 1, 10, 6, 7, 8, 9):
        loads[k].start()

    def remote(phase, src, dst, to):
        pltpu.make_async_remote_copy(
            src_ref=src,
            dst_ref=dst,
            send_sem=send_sems.at[phase],
            recv_sem=recv_sems.at[phase],
            device_id=place_of(to)[1],
            device_id_type=MESH,
        ).start()

    def exchange(phase, src, dst):
        for t in peers:
            remote(phase, src.at[place_of(t)[0]], dst.at[me], t)
        dst[me] = src[me]

    def wait_for(sems, phase, ref):
        pltpu.make_async_copy(ref, ref, sems.at[phase]).wait()

    def arrived(phase, dst):
        wait_for(recv_sems, phase, dst.at[pl.ds(0, n - 1)])

    def sent(phase, dst):
        wait_for(send_sems, phase, dst.at[pl.ds(0, n - 1)])

    my_chip = me // 2
    my_core = lax.rem(me, 2)

    def spread(phase, ref):
        for t in peers:
            if t % 2 == 0:
                mine = ref.at[my_chip, my_core]
                remote(phase, mine, mine, t)

    def same_core(ref):
        return ref.at[pl.ds(0, n // 2 - 1), 0]

    def hand_over(phase, ref):
        mine = ref.at[:, my_core]
        remote(phase, mine, mine, 1)

    def part_of(held_by, first, last):
        return blocks.at[me ^ held_by, pl.ds(first, last - first)]

    here = {0}

    def ensure(block):
        if block in here:
            return
        here.add(block)
        for slot, (_, source, to, first, last) in enumerate(plan):
            if source ^ to == block:
                wait_for(plan_recv, slot, part_of(block, first, last))

    def gather(stage):
        for slot, (when, source, to, first, last) in enumerate(plan):
            if when == stage:
                ensure(source)
                part = part_of(source, first, last)
                pltpu.make_async_remote_copy(
                    src_ref=part,
                    dst_ref=part,
                    send_sem=plan_send.at[slot],
                    recv_sem=plan_recv.at[slot],
                    device_id=place_of(to)[1],
                    device_id_type=MESH,
                ).start()

    def load_cells(ref):
        return jnp.concatenate(
            [ref[i, pl.ds(p, n, stride=rows), :] for i in range(rows) for p in range(rows)], 0
        )

    def store_cells(ref, value):
        for i in range(rows):
            for p in range(rows):
                at = i * length + p * n
                ref[i, pl.ds(p, n, stride=rows), :] = value[at : at + n]

    def split_h(value):
        return value.T.reshape(n, own, cells)

    def merge_h(value):
        return value.reshape(hidden, cells).T

    def stack(value):
        return jnp.concatenate([value[:, i * length : (i + 1) * length] for i in range(rows)], 0)

    def unstack(value):
        return jnp.concatenate([value[i * n : (i + 1) * n] for i in range(rows)], 1)

    def bias(first, last):
        return jnp.concatenate([b_ref[k : k + 1] for k in range(first, last)], 1)

    natural = lax.broadcasted_iota(jnp.int32, (length, length), 0)
    place = lax.broadcasted_iota(jnp.int32, (length, length), 1)
    order = jnp.where(natural == lax.rem(place, n) * rows + place // n, 1.0, 0.0)
    loads[1].wait()
    keep = lax.dot_general(
        mask_ref[...].astype(jnp.bfloat16),
        order.astype(jnp.bfloat16),
        (NN, ((), ())),
        preferred_element_type=jnp.float32,
    )
    keep = jnp.concatenate([keep[i : i + 1] for i in range(rows)], 1)

    loads[0].wait()
    loads[2].wait()
    loads[3].wait()
    pair_hat, pair_scale = normalise(load_cells(pair_ref))
    normed = pair_hat * gin_ref[...] + bin_ref[...]
    width = 4 * hidden
    lanes = b_ref.shape[1]
    loads[4].wait()
    loads[5].wait()
    pieces = dot(normed, win_ref[:, :width], NN) + bias(0, width // lanes)
    p1 = jax.nn.sigmoid(pieces[:, :hidden])
    p2 = pieces[:, hidden : 2 * hidden]
    p3 = jax.nn.sigmoid(pieces[:, 2 * hidden : 3 * hidden])
    p4 = pieces[:, 3 * hidden :]
    keep_tall = jnp.broadcast_to(keep, (hidden, cells)).T
    left = keep_tall * p1 * p2
    right = keep_tall * p3 * p4
    send1[:, :own, :] = split_h(left)
    send1[:, own:, :] = split_h(right)
    blocks[me, :cells, :] = normed
    for q in range(8):
        at = min(q, cells // channels - 1) * channels
        blocks[me, cells + q : cells + q + 1, :] = keep[:, at : at + channels]
    pl.semaphore_wait(barrier, n - 1)
    exchange(0, send1, recv1)
    gather(0)

    for q, k in enumerate((0, 2)):
        at = k * hidden
        weights_t[q] = win_ref[:, at : at + hidden].T.reshape(n, own, channels)
        column = b_ref[at // lanes : at // lanes + 1]
        bias_t[q] = jnp.broadcast_to(column, (lanes, hidden)).T.reshape(n, own, lanes)

    gate = jax.nn.sigmoid(dot(normed, win_ref[:, width:], NN) + bias(width // lanes, b_ref.shape[0]))
    for k in range(6, 11):
        loads[k].wait()
    cot = load_cells(cot_ref)

    arrived(0, recv1)
    lefts = [stack(recv1[:, h, :]) for h in range(own)]
    rights = [stack(recv1[:, own + h, :]) for h in range(own)]
    for h in range(own):
        send2[:, h, :] = unstack(dot(lefts[h], rights[h], NT))
    exchange(1, send2, recv2)
    gather(1)
    arrived(1, recv2)

    prod_hat, prod_scale = normalise(merge_h(recv2[...]))
    normed_product = prod_hat * gout_ref[...] + bout_ref[...]
    projected = dot(normed_product, wout_ref[...], NN) + bo_ref[...]
    d_out = cot * gate
    d_product = normalise_back(
        prod_hat, prod_scale, dot(d_out, wout_ref[...], NT) * gout_ref[...]
    )
    send3[...] = split_h(d_product)
    exchange(2, send3, recv3)
    gather(2)

    store_cells(update_ref, gate * projected)
    d_gate = cot * projected * gate * (1.0 - gate)
    d_wout = dot(normed_product, d_out, TN)
    d_wgate = dot(normed, d_gate, TN)
    send4[:, :, :own, :] = d_wgate.reshape(n // 2, 2, own, channels)
    send4[:, :, own:, :] = d_wout.reshape(n // 2, 2, own, channels)
    remote(7, send4.at[:, 1 - my_core], pair4, 1)
    d_normed = dot(d_gate, win_ref[:, width:], NT)
    wait_for(recv_sems, 7, pair4)
    sum4[...] = send4[:, my_core] + pair4[...]
    for t in peers:
        if t % 2 == 0:
            remote(3, sum4.at[place_of(t)[0] // 2], recv4.at[my_chip], t)
    recv4[my_chip] = sum4[my_chip]

    gate_weights = halves(jnp.concatenate([weights_t[0, me], weights_t[1, me]], 0))
    gate_bias = jnp.concatenate([bias_t[0, me], bias_t[1, me]], 0)[:, :1]

    def keep_of(d):
        return jnp.concatenate(
            [blocks[d, cells + q : cells + q + 1, :] for q in range(cells // channels)], 1
        )

    def side_by_side(take, offsets):
        return jnp.concatenate([take(me ^ t) for t in offsets], 1)

    def block_halves(offsets):
        return halves(jnp.concatenate([blocks[me ^ t, :cells, :] for t in offsets], 0))

    def factors_of(offsets, x):
        gates = jax.nn.sigmoid(dot_halves(gate_weights, x, NT) + gate_bias)
        values = side_by_side(lambda d: recv1[d], offsets)
        present = side_by_side(keep_of, offsets)
        return jnp.concatenate([values * (1.0 - gates), present * gates], 0)

    def grads_of(offsets, x, scaled):
        grads = side_by_side(lambda d: send5[d], offsets)
        return dot_halves(halves(jnp.concatenate([grads, grads], 0) * scaled), x, NN)

    def came_in(stage):
        return sorted({e[1] ^ e[2] for e in plan if e[0] == stage})

    first_ones = [0, *came_in(0), *came_in(1)]
    for block in first_ones:
        ensure(block)
    first_factors = factors_of(first_ones, block_halves(first_ones))
    for at, t in enumerate(first_ones):
        factors[me ^ t] = first_factors[:, at * cells : (at + 1) * cells]

    arrived(2, recv3)
    d_cols = [stack(recv3[:, h, :]) for h in range(own)]
    for h in range(own):
        send5[:, h, :] = unstack(dot(d_cols[h], rights[h], NN))
    for h in range(own):
        send5[:, own + h, :] = unstack(dot(d_cols[h], lefts[h], TN))
    exchange(4, send5, recv5)
    gather(3)
    total = grads_of(
        first_ones, block_halves(first_ones), side_by_side(lambda d: factors[d], first_ones)
    )
    wait_for(recv_sems, 3, recv4.at[pl.ds(0, n // 2 - 1)])
    early[my_chip, my_core] = jnp.sum(recv4[...], 0) / length
    spread(8, early)
    for stage in (2, 3):
        for block in came_in(stage):
            ensure(block)
        x = block_halves(came_in(stage))
        total = total + grads_of(came_in(stage), x, factors_of(came_in(stage), x))
    late[my_chip, my_core] = total / length
    spread(5, late)

    arrived(4, recv5)
    half = 2 * hidden
    d_left = merge_h(recv5[:, :own, :]) * keep_tall
    d_first = jnp.concatenate([d_left * p2 * p1 * (1.0 - p1), d_left * p1], 1)
    d_normed = d_normed + dot(d_first, win_ref[:, :half], NT)
    d_right = merge_h(recv5[:, own:, :]) * keep_tall
    d_second = jnp.concatenate([d_right * p4 * p3 * (1.0 - p3), d_right * p3], 1)
    d_normed = d_normed + dot(d_second, win_ref[:, half:width], NT)
    store_cells(gpair_ref, normalise_back(pair_hat, pair_scale, d_normed * gin_ref[...]))

    wait_for(recv_sems, 8, same_core(early))
    hand_over(9, early)
    for phase, ref in ((0, recv1), (1, recv2), (2, recv3), (4, recv5)):
        sent(phase, ref)
    wait_for(send_sems, 3, recv4.at[pl.ds(0, n // 2 - 1)])
    wait_for(send_sems, 7, pair4)
    for slot, (_, source, _, first, last) in enumerate(plan):
        wait_for(plan_send, slot, part_of(source, first, last))
    wait_for(send_sems, 8, same_core(early))
    wait_for(recv_sems, 5, same_core(late))
    hand_over(6, late)
    wait_for(recv_sems, 9, early.at[:, 0])
    gwin_ref[:, width:] = early[:, :, :own, :].reshape(channels, channels)
    gwout_ref[...] = early[:, :, own:, :].reshape(hidden, channels)
    wait_for(recv_sems, 6, late.at[:, 0])
    for q, k in enumerate((0, 2, 1, 3)):
        piece = late[:, :, q * own : (q + 1) * own, :].reshape(hidden, channels)
        gwin_ref[:, k * hidden : (k + 1) * hidden] = piece.T

    wait_for(send_sems, 5, same_core(late))
    for phase, ref in ((9, early), (6, late)):
        wait_for(send_sems, phase, ref.at[:, 0])


def write_out(a, b, c, d, a_out, b_out, c_out, d_out, sems):
    pairs = ((a, a_out), (b, b_out), (c, c_out), (d, d_out))
    copies = [pltpu.make_async_copy(x, y, sems.at[k]) for k, (x, y) in enumerate(pairs)]
    for copy in copies:
        copy.start()
    for copy in copies:
        copy.wait()


def on_device(
    n_row,
    n_ch,
    pair_rep,
    pair_mask,
    ln_in_gain,
    ln_in_bias,
    w_in,
    b_in,
    ln_out_gain,
    ln_out_bias,
    w_out,
    b_out,
    cotangent,
):
    n = n_row * n_ch
    rows, length, channels = pair_rep.shape
    hidden = w_out.shape[0]
    own = hidden // n
    cells = rows * length
    f32 = jnp.float32

    def both(*shape):
        return [pltpu.VMEM((n, *shape), f32), pltpu.VMEM((n, *shape), f32)]

    inputs = (
        pair_rep,
        pair_mask,
        ln_in_gain[None],
        ln_in_bias[None],
        w_in,
        b_in.reshape(-1, min(128, hidden)),
        ln_out_gain[None],
        ln_out_bias[None],
        w_out,
        b_out[None],
        cotangent,
    )
    lanes = min(128, hidden)
    plan = gather_plan(n, n_ch, cells + 8)
    anywhere = pl.BlockSpec(memory_space=pl.ANY)
    vmem = pl.BlockSpec(memory_space=pltpu.VMEM)
    inputs = tuple(pltpu.with_memory_space_constraint(x, pltpu.MemorySpace.HBM) for x in inputs)
    out_shape = tuple(
        jax.ShapeDtypeStruct(x.shape, f32) for x in (pair_rep, pair_rep, w_in, w_out)
    )
    parts = pl.pallas_call(
        functools.partial(kernel, n_row, n_ch, plan),
        out_shape=out_shape,
        in_specs=[anywhere] * 11,
        out_specs=(vmem,) * 4,
        scratch_shapes=[
            *[pltpu.VMEM(x.shape, x.dtype) for x in inputs],
            *both(2 * own, cells),
            *both(own, cells),
            *both(own, cells),
            pltpu.VMEM((n // 2, 2, 2 * own, channels), f32),
            *[pltpu.VMEM((n // 2, 2 * own, channels), f32)] * 3,
            *both(2 * own, cells),
            pltpu.VMEM((n // 2, 2, 2 * own, channels), f32),
            pltpu.VMEM((n // 2, 2, 4 * own, channels), f32),
            pltpu.VMEM((n, 4 * own, cells), f32),
            pltpu.VMEM((n, cells + 8, channels), f32),
            pltpu.VMEM((2, n, own, channels), f32),
            pltpu.VMEM((2, n, own, lanes), f32),
            pltpu.SemaphoreType.DMA((10,)),
            pltpu.SemaphoreType.DMA((10,)),
            pltpu.SemaphoreType.DMA((len(plan),)),
            pltpu.SemaphoreType.DMA((len(plan),)),
            pltpu.SemaphoreType.DMA((11,)),
        ],
        compiler_params=pltpu.CompilerParams(
            collective_id=0,
            has_side_effects=True,
            vmem_limit_bytes=n * (cells + 8) * channels * 4 + (22 << 20),
        ),
    )(*inputs)
    return pl.pallas_call(
        write_out,
        out_shape=out_shape,
        in_specs=[vmem] * 4,
        out_specs=(anywhere,) * 4,
        scratch_shapes=[pltpu.SemaphoreType.DMA((4,))],
        compiler_params=pltpu.CompilerParams(vmem_limit_bytes=8 << 20),
    )(*parts)


def solution(mesh):
    rows = P(("row", "ch"), None, None)
    placed = (rows, P(("row", "ch"), None), P(), P(), P(), P(), P(), P(), P(), P(), rows)
    return jax.shard_map(
        functools.partial(on_device, mesh.shape["row"], mesh.shape["ch"]),
        mesh=mesh,
        in_specs=placed,
        out_specs=(rows, rows, P(), P()),
        check_vma=False,
    )
```

```python
import functools

import jax
import jax.numpy as jnp
from jax import lax
from jax.experimental import pallas as pl
from jax.experimental.pallas import tpu as pltpu
from jax.sharding import PartitionSpec as P

epsilon = 1e-05
MESH = pl.DeviceIdType.MESH


def halves(a):
    high = a.astype(jnp.bfloat16)
    return high, (a - high.astype(jnp.float32)).astype(jnp.bfloat16)


def dot_halves(a, b, contract):
    def one(x, y):
        return lax.dot_general(
            x, y, (contract, ((), ())), preferred_element_type=jnp.float32
        )

    (a_high, a_low), (b_high, b_low) = a, b
    return one(a_high, b_low) + one(a_low, b_high) + one(a_high, b_high)


def dot(a, b, contract):
    return dot_halves(halves(a), halves(b), contract)


NN = ((1,), (0,))
NT = ((1,), (1,))
TN = ((0,), (0,))


def normalise(x):
    center = jnp.mean(x, -1, keepdims=True)
    spread = jnp.mean((x - center) ** 2, -1, keepdims=True)
    scale = lax.rsqrt(spread + epsilon)
    return (x - center) * scale, scale


def normalise_back(x_hat, scale, d_hat):
    return scale * (
        d_hat
        - jnp.mean(d_hat, -1, keepdims=True)
        - x_hat * jnp.mean(d_hat * x_hat, -1, keepdims=True)
    )


def farthest_first(n, n_ch):
    assert n & (n - 1) == 0

    def hops(t):
        row, ch = divmod(t, n_ch)
        return (row // 2).bit_length() + row % 2 + ch // 2

    return sorted(range(1, n), key=lambda t: (-hops(t), t % 2, t))


def gather_plan(n, n_ch, rows):
    core, side, up = 1, n_ch // 2, n_ch
    middle = rows // 16 * 8
    plan = []
    for z in range(0, n, 2 * n_ch):
        low = z & -z
        stage = 0 if z == 0 else 1 if z == low else 2
        if stage == 1:
            plan.append((0, 0, z, 0, rows))
        if stage == 2:
            near = z ^ low
            forwards = near & (near - 1) == 0
            plan.append((1, near, low, 0, rows) if forwards else (1, 0, z, 0, rows))
        plan.append((stage, z, side, 0, rows))
        plan.append((stage, z, up, 0, rows))
        if stage == 0:
            plan.append((0, 0, side ^ up, 0, rows))
        elif stage < 2:
            plan.append((stage + 1, z ^ side, up, 0, middle))
            plan.append((stage + 1, z ^ up, side, middle, rows))
        else:
            plan.append((1, side ^ up, z, 0, rows))
        plan.append((stage, z, core, 0, rows))
        plan.append((stage + 1, z ^ side, core, 0, rows))
        plan.append((stage + 1, z ^ up, core, 0, rows))
        plan.append((1 if z == 0 else min(stage + 2, 3), z ^ side ^ up, core, 0, rows))
    return sorted(plan, key=lambda e: (e[0], e[2] == core, e[1] > 2 * n_ch and e[2] < 2 * n_ch))


def kernel(
    n_row,
    n_ch,
    plan,
    *refs,
):
    inputs, rest = refs[:11], refs[11:]
    update_ref, gpair_ref, gwin_ref, gwout_ref = rest[:4]
    held, rest = rest[4:15], rest[15:]
    (
        pair_ref,
        mask_ref,
        gin_ref,
        bin_ref,
        win_ref,
        b_ref,
        gout_ref,
        bout_ref,
        wout_ref,
        bo_ref,
        cot_ref,
    ) = held
    (
        send1,
        recv1,
        send2,
        recv2,
        send3,
        recv3,
        send4,
        pair4,
        sum4,
        recv4,
        send5,
        recv5,
        early,
        late,
        factors,
        blocks,
        weights_t,
        bias_t,
        send_sems,
        recv_sems,
        plan_send,
        plan_recv,
        load_sems,
    ) = rest
    n = n_row * n_ch
    rows, length, channels = pair_ref.shape
    hidden = wout_ref.shape[0]
    own = hidden // n
    cells = rows * length
    my_row = lax.axis_index("row")
    my_ch = lax.axis_index("ch")
    me = my_row * n_ch + my_ch
    peers = farthest_first(n, n_ch)

    def place_of(t):
        d = me ^ t
        return d, (d // n_ch, lax.rem(d, n_ch))

    barrier = pltpu.get_barrier_semaphore()
    for t in peers:
        pl.semaphore_signal(barrier, inc=1, device_id=place_of(t)[1], device_id_type=MESH)

    loads = [
        pltpu.make_async_copy(inputs[k], held[k], load_sems.at[k]) for k in range(len(inputs))
    ]
    for k in (0, 2, 3, 4, 5, 1, 10, 6, 7, 8, 9):
        loads[k].start()

    def remote(phase, src, dst, to):
        pltpu.make_async_remote_copy(
            src_ref=src,
            dst_ref=dst,
            send_sem=send_sems.at[phase],
            recv_sem=recv_sems.at[phase],
            device_id=place_of(to)[1],
            device_id_type=MESH,
        ).start()

    def exchange(phase, src, dst):
        for t in peers:
            remote(phase, src.at[place_of(t)[0]], dst.at[me], t)
        dst[me] = src[me]

    def wait_for(sems, phase, ref):
        pltpu.make_async_copy(ref, ref, sems.at[phase]).wait()

    def arrived(phase, dst):
        wait_for(recv_sems, phase, dst.at[pl.ds(0, n - 1)])

    def sent(phase, dst):
        wait_for(send_sems, phase, dst.at[pl.ds(0, n - 1)])

    my_chip = me // 2
    my_core = lax.rem(me, 2)

    def spread(phase, ref):
        for t in peers:
            if t % 2 == 0:
                mine = ref.at[my_chip, my_core]
                remote(phase, mine, mine, t)

    def same_core(ref):
        return ref.at[pl.ds(0, n // 2 - 1), 0]

    def hand_over(phase, ref):
        mine = ref.at[:, my_core]
        remote(phase, mine, mine, 1)

    def part_of(held_by, first, last):
        return blocks.at[me ^ held_by, pl.ds(first, last - first)]

    here = {0}

    def ensure(block):
        if block in here:
            return
        here.add(block)
        for slot, (_, source, to, first, last) in enumerate(plan):
            if source ^ to == block:
                wait_for(plan_recv, slot, part_of(block, first, last))

    def gather(stage):
        for slot, (when, source, to, first, last) in enumerate(plan):
            if when == stage:
                ensure(source)
                part = part_of(source, first, last)
                pltpu.make_async_remote_copy(
                    src_ref=part,
                    dst_ref=part,
                    send_sem=plan_send.at[slot],
                    recv_sem=plan_recv.at[slot],
                    device_id=place_of(to)[1],
                    device_id_type=MESH,
                ).start()

    def load_cells(ref):
        return jnp.concatenate(
            [ref[i, pl.ds(p, n, stride=rows), :] for i in range(rows) for p in range(rows)], 0
        )

    def store_cells(ref, value):
        for i in range(rows):
            for p in range(rows):
                at = i * length + p * n
                ref[i, pl.ds(p, n, stride=rows), :] = value[at : at + n]

    def split_h(value):
        return value.T.reshape(n, own, cells)

    def merge_h(value):
        return value.reshape(hidden, cells).T

    def stack(value):
        return jnp.concatenate([value[:, i * length : (i + 1) * length] for i in range(rows)], 0)

    def unstack(value):
        return jnp.concatenate([value[i * n : (i + 1) * n] for i in range(rows)], 1)

    def bias(first, last):
        return jnp.concatenate([b_ref[k : k + 1] for k in range(first, last)], 1)

    natural = lax.broadcasted_iota(jnp.int32, (length, length), 0)
    place = lax.broadcasted_iota(jnp.int32, (length, length), 1)
    order = jnp.where(natural == lax.rem(place, n) * rows + place // n, 1.0, 0.0)
    loads[1].wait()
    keep = lax.dot_general(
        mask_ref[...].astype(jnp.bfloat16),
        order.astype(jnp.bfloat16),
        (NN, ((), ())),
        preferred_element_type=jnp.float32,
    )
    keep = jnp.concatenate([keep[i : i + 1] for i in range(rows)], 1)

    loads[0].wait()
    loads[2].wait()
    loads[3].wait()
    pair_hat, pair_scale = normalise(load_cells(pair_ref))
    normed = pair_hat * gin_ref[...] + bin_ref[...]
    width = 4 * hidden
    lanes = b_ref.shape[1]
    loads[4].wait()
    loads[5].wait()
    pieces = dot(normed, win_ref[:, :width], NN) + bias(0, width // lanes)
    p1 = jax.nn.sigmoid(pieces[:, :hidden])
    p2 = pieces[:, hidden : 2 * hidden]
    p3 = jax.nn.sigmoid(pieces[:, 2 * hidden : 3 * hidden])
    p4 = pieces[:, 3 * hidden :]
    keep_tall = jnp.broadcast_to(keep, (hidden, cells)).T
    left = keep_tall * p1 * p2
    right = keep_tall * p3 * p4
    send1[:, :own, :] = split_h(left)
    send1[:, own:, :] = split_h(right)
    blocks[me, :cells, :] = normed
    for q in range(8):
        at = min(q, cells // channels - 1) * channels
        blocks[me, cells + q : cells + q + 1, :] = keep[:, at : at + channels]
    pl.semaphore_wait(barrier, n - 1)
    exchange(0, send1, recv1)
    gather(0)

    for q, k in enumerate((0, 2)):
        at = k * hidden
        weights_t[q] = win_ref[:, at : at + hidden].T.reshape(n, own, channels)
        column = b_ref[at // lanes : at // lanes + 1]
        bias_t[q] = jnp.broadcast_to(column, (lanes, hidden)).T.reshape(n, own, lanes)

    gate = jax.nn.sigmoid(dot(normed, win_ref[:, width:], NN) + bias(width // lanes, b_ref.shape[0]))
    for k in range(6, 11):
        loads[k].wait()
    cot = load_cells(cot_ref)

    arrived(0, recv1)
    lefts = [stack(recv1[:, h, :]) for h in range(own)]
    rights = [stack(recv1[:, own + h, :]) for h in range(own)]
    for h in range(own):
        send2[:, h, :] = unstack(dot(lefts[h], rights[h], NT))
    exchange(1, send2, recv2)
    gather(1)
    arrived(1, recv2)

    prod_hat, prod_scale = normalise(merge_h(recv2[...]))
    normed_product = prod_hat * gout_ref[...] + bout_ref[...]
    projected = dot(normed_product, wout_ref[...], NN) + bo_ref[...]
    d_out = cot * gate
    d_product = normalise_back(
        prod_hat, prod_scale, dot(d_out, wout_ref[...], NT) * gout_ref[...]
    )
    send3[...] = split_h(d_product)
    exchange(2, send3, recv3)
    gather(2)

    store_cells(update_ref, gate * projected)
    d_gate = cot * projected * gate * (1.0 - gate)
    d_wout = dot(normed_product, d_out, TN)
    d_wgate = dot(normed, d_gate, TN)
    send4[:, :, :own, :] = d_wgate.reshape(n // 2, 2, own, channels)
    send4[:, :, own:, :] = d_wout.reshape(n // 2, 2, own, channels)
    remote(7, send4.at[:, 1 - my_core], pair4, 1)
    d_normed = dot(d_gate, win_ref[:, width:], NT)
    wait_for(recv_sems, 7, pair4)
    sum4[...] = send4[:, my_core] + pair4[...]
    for t in peers:
        if t % 2 == 0:
            remote(3, sum4.at[place_of(t)[0] // 2], recv4.at[my_chip], t)
    recv4[my_chip] = sum4[my_chip]

    gate_weights = halves(jnp.concatenate([weights_t[0, me], weights_t[1, me]], 0))
    gate_bias = jnp.concatenate([bias_t[0, me], bias_t[1, me]], 0)[:, :1]

    def keep_of(d):
        return jnp.concatenate(
            [blocks[d, cells + q : cells + q + 1, :] for q in range(cells // channels)], 1
        )

    def side_by_side(take, offsets):
        return jnp.concatenate([take(me ^ t) for t in offsets], 1)

    def block_halves(offsets):
        return halves(jnp.concatenate([blocks[me ^ t, :cells, :] for t in offsets], 0))

    def factors_of(offsets, x):
        gates = jax.nn.sigmoid(dot_halves(gate_weights, x, NT) + gate_bias)
        values = side_by_side(lambda d: recv1[d], offsets)
        present = side_by_side(keep_of, offsets)
        return jnp.concatenate([values * (1.0 - gates), present * gates], 0)

    def grads_of(offsets, x, scaled):
        grads = side_by_side(lambda d: send5[d], offsets)
        return dot_halves(halves(jnp.concatenate([grads, grads], 0) * scaled), x, NN)

    def came_in(stage):
        return sorted({e[1] ^ e[2] for e in plan if e[0] == stage})

    first_ones = [0, *came_in(0), *came_in(1)]
    for block in first_ones:
        ensure(block)
    first_factors = factors_of(first_ones, block_halves(first_ones))
    for at, t in enumerate(first_ones):
        factors[me ^ t] = first_factors[:, at * cells : (at + 1) * cells]

    arrived(2, recv3)
    d_cols = [stack(recv3[:, h, :]) for h in range(own)]
    for h in range(own):
        send5[:, h, :] = unstack(dot(d_cols[h], rights[h], NN))
    for h in range(own):
        send5[:, own + h, :] = unstack(dot(d_cols[h], lefts[h], TN))
    exchange(4, send5, recv5)
    wait_for(recv_sems, 3, recv4.at[pl.ds(0, n // 2 - 1)])
    early[my_chip, my_core] = jnp.sum(recv4[...], 0) / length
    spread(8, early)
    gather(3)
    total = grads_of(
        first_ones, block_halves(first_ones), side_by_side(lambda d: factors[d], first_ones)
    )
    for stage in (2, 3):
        for block in came_in(stage):
            ensure(block)
        x = block_halves(came_in(stage))
        total = total + grads_of(came_in(stage), x, factors_of(came_in(stage), x))
    late[my_chip, my_core] = total / length
    spread(5, late)

    arrived(4, recv5)
    half = 2 * hidden
    d_left = merge_h(recv5[:, :own, :]) * keep_tall
    d_first = jnp.concatenate([d_left * p2 * p1 * (1.0 - p1), d_left * p1], 1)
    d_normed = d_normed + dot(d_first, win_ref[:, :half], NT)
    d_right = merge_h(recv5[:, own:, :]) * keep_tall
    d_second = jnp.concatenate([d_right * p4 * p3 * (1.0 - p3), d_right * p3], 1)
    d_normed = d_normed + dot(d_second, win_ref[:, half:width], NT)
    store_cells(gpair_ref, normalise_back(pair_hat, pair_scale, d_normed * gin_ref[...]))

    wait_for(recv_sems, 8, same_core(early))
    hand_over(9, early)
    for phase, ref in ((0, recv1), (1, recv2), (2, recv3), (4, recv5)):
        sent(phase, ref)
    wait_for(send_sems, 3, recv4.at[pl.ds(0, n // 2 - 1)])
    wait_for(send_sems, 7, pair4)
    for slot, (_, source, _, first, last) in enumerate(plan):
        wait_for(plan_send, slot, part_of(source, first, last))
    wait_for(send_sems, 8, same_core(early))
    wait_for(recv_sems, 5, same_core(late))
    hand_over(6, late)
    wait_for(recv_sems, 9, early.at[:, 0])
    gwin_ref[:, width:] = early[:, :, :own, :].reshape(channels, channels)
    gwout_ref[...] = early[:, :, own:, :].reshape(hidden, channels)
    wait_for(recv_sems, 6, late.at[:, 0])
    for q, k in enumerate((0, 2, 1, 3)):
        piece = late[:, :, q * own : (q + 1) * own, :].reshape(hidden, channels)
        gwin_ref[:, k * hidden : (k + 1) * hidden] = piece.T

    wait_for(send_sems, 5, same_core(late))
    for phase, ref in ((9, early), (6, late)):
        wait_for(send_sems, phase, ref.at[:, 0])


def write_out(a, b, c, d, a_out, b_out, c_out, d_out, sems):
    pairs = ((a, a_out), (b, b_out), (c, c_out), (d, d_out))
    copies = [pltpu.make_async_copy(x, y, sems.at[k]) for k, (x, y) in enumerate(pairs)]
    for copy in copies:
        copy.start()
    for copy in copies:
        copy.wait()


def on_device(
    n_row,
    n_ch,
    pair_rep,
    pair_mask,
    ln_in_gain,
    ln_in_bias,
    w_in,
    b_in,
    ln_out_gain,
    ln_out_bias,
    w_out,
    b_out,
    cotangent,
):
    n = n_row * n_ch
    rows, length, channels = pair_rep.shape
    hidden = w_out.shape[0]
    own = hidden // n
    cells = rows * length
    f32 = jnp.float32

    def both(*shape):
        return [pltpu.VMEM((n, *shape), f32), pltpu.VMEM((n, *shape), f32)]

    inputs = (
        pair_rep,
        pair_mask,
        ln_in_gain[None],
        ln_in_bias[None],
        w_in,
        b_in.reshape(-1, min(128, hidden)),
        ln_out_gain[None],
        ln_out_bias[None],
        w_out,
        b_out[None],
        cotangent,
    )
    lanes = min(128, hidden)
    plan = gather_plan(n, n_ch, cells + 8)
    anywhere = pl.BlockSpec(memory_space=pl.ANY)
    vmem = pl.BlockSpec(memory_space=pltpu.VMEM)
    inputs = tuple(pltpu.with_memory_space_constraint(x, pltpu.MemorySpace.HBM) for x in inputs)
    out_shape = tuple(
        jax.ShapeDtypeStruct(x.shape, f32) for x in (pair_rep, pair_rep, w_in, w_out)
    )
    parts = pl.pallas_call(
        functools.partial(kernel, n_row, n_ch, plan),
        out_shape=out_shape,
        in_specs=[anywhere] * 11,
        out_specs=(vmem,) * 4,
        scratch_shapes=[
            *[pltpu.VMEM(x.shape, x.dtype) for x in inputs],
            *both(2 * own, cells),
            *both(own, cells),
            *both(own, cells),
            pltpu.VMEM((n // 2, 2, 2 * own, channels), f32),
            *[pltpu.VMEM((n // 2, 2 * own, channels), f32)] * 3,
            *both(2 * own, cells),
            pltpu.VMEM((n // 2, 2, 2 * own, channels), f32),
            pltpu.VMEM((n // 2, 2, 4 * own, channels), f32),
            pltpu.VMEM((n, 4 * own, cells), f32),
            pltpu.VMEM((n, cells + 8, channels), f32),
            pltpu.VMEM((2, n, own, channels), f32),
            pltpu.VMEM((2, n, own, lanes), f32),
            pltpu.SemaphoreType.DMA((10,)),
            pltpu.SemaphoreType.DMA((10,)),
            pltpu.SemaphoreType.DMA((len(plan),)),
            pltpu.SemaphoreType.DMA((len(plan),)),
            pltpu.SemaphoreType.DMA((11,)),
        ],
        compiler_params=pltpu.CompilerParams(
            collective_id=0,
            has_side_effects=True,
            vmem_limit_bytes=n * (cells + 8) * channels * 4 + (22 << 20),
        ),
    )(*inputs)
    return pl.pallas_call(
        write_out,
        out_shape=out_shape,
        in_specs=[vmem] * 4,
        out_specs=(anywhere,) * 4,
        scratch_shapes=[pltpu.SemaphoreType.DMA((4,))],
        compiler_params=pltpu.CompilerParams(vmem_limit_bytes=8 << 20),
    )(*parts)


def solution(mesh):
    rows = P(("row", "ch"), None, None)
    placed = (rows, P(("row", "ch"), None), P(), P(), P(), P(), P(), P(), P(), P(), rows)
    return jax.shard_map(
        functools.partial(on_device, mesh.shape["row"], mesh.shape["ch"]),
        mesh=mesh,
        in_specs=placed,
        out_specs=(rows, rows, P(), P()),
        check_vma=False,
    )
```
